512 devices in a mesh: mode: 8 (over x, core), slab: 64 (over z, y).
Axes of the slice: x: 4, y: 8, z: 8, core: 2. Of those that a mesh axis runs over, the one named last changes fastest.
Arguments:
- log_cond: float32 [256, 128, 128], P('slab'), may hold values from -1 to 1
- head_slope: float32 [256, 128, 128], P('slab'), may hold values from -6 to 6
- modes: bfloat16 [64, 256, 128, 128], P('mode', 'slab'), may hold values from -6 to 6
- obs_cells: int32 [65536], P('slab'), may hold values from 0 to 65535
- obs_var: float32 [65536], P('slab'), may hold values from 0.2 to 2
- misfit: float32 [65536, 16], P('slab'), may hold values from -24 to 24
- base_fields: bfloat16 [16, 256, 128, 128], P(None, 'slab', 'mode'), may hold values from -6 to 6
Outputs:
- fields: float32 [16, 256, 128, 128], P(None, 'slab', 'mode')
The draws below stay inside these ranges and needn't reach their ends.
Inputs may be any that keep to these rules, and one draw needn't show every extreme that they name: `obs_cells`: entry o names a cell of the planes (o // 1024) * 4 to (o // 1024 + 1) * 4 - 1, counted from the first of them: value c stands for plane (o // 1024) * 4 + c // 16384, first horizontal index (c // 128) % 128, second c % 128; cells may repeat.
All inputs are finite; a program needn't handle non-finite values.
Results may differ from the reference program's by a relative error of at most 0.0003.
Values may be sent and summed in bfloat16 or wider, within the bound.
No kernel may reach another device: no remote copies, remote signals or barrier semaphores. Data moves between devices by JAX's collectives and lax.ppermute only.
A program may use at most 128 MiB of HBM per device.

```python
import math
import jax
import jax.numpy as jnp
from jax import lax

NX = 128
NY = 128
CZ = 4
MODES = 64
FIELDS = 16
ITERS = 3
OBS_SLAB = 1024
OBS = 65536
NZ = 256


def place_ends(values, rng, smallest, high):
    extent = values.shape
    place = [jax.random.randint(jax.random.fold_in(rng, axis), (), 0, extent[axis]) for axis in range(len(extent))]
    values = values.at[tuple(place)].set(smallest)
    longest = extent.index(max(extent))
    place[longest] = (place[longest] + 1) % extent[longest]
    return values.at[tuple(place)].set(high)


def shard_levels(rng, extent, pieces, smallest, high):
    level = 1.0
    for dim, parts in pieces:
        heights = jax.random.uniform(jax.random.fold_in(jax.random.fold_in(rng, 6), dim), (parts,), jnp.float32, smallest / len(pieces), high / len(pieces))
        level = level * jnp.repeat(jnp.exp(heights), extent[dim] // parts).reshape((-1,) + (1,) * (len(extent) - 1 - dim))
    return level


def normal_values(own_key, shape, deviation, limit, cuts=(), kind=jnp.bfloat16):
    level = shard_levels(own_key, shape, cuts, -0.22, 0.18) if cuts else 1.0
    values = jax.random.normal(own_key, shape, jnp.float32) * deviation * level
    return jnp.minimum(jnp.maximum(values, -limit), limit).astype(kind)


def setup_inputs(seed: int = 0) -> dict:
    keys = jax.random.split(jax.random.key(seed), 8)
    return {
        "log_cond": jnp.clip(jax.random.uniform(keys[0], (NZ, NX, NY), jnp.float32, -1.0, 1.0) * shard_levels(keys[0], (NZ, NX, NY), ((0, 64),), -0.4, 0.0), -1.0, 1.0),
        "head_slope": normal_values(keys[1], (NZ, NX, NY), 1.0, 6.0, ((0, 64),), jnp.float32),
        "modes": normal_values(keys[2], (MODES, NZ, NX, NY), 1.0, 6.0, ((0, 8), (1, 64))),
        "obs_cells": place_ends(jax.random.randint(keys[3], (OBS,), 0, CZ * NX * NY), jax.random.fold_in(keys[3], 1), 0, (CZ * NX * NY) - 1).astype(jnp.int32),
        "obs_var": jnp.clip(jnp.exp(math.log(2.0) - 2.3025851 * jax.random.uniform(keys[4], (OBS,), jnp.float32) ** shard_levels(keys[4], (OBS,), ((0, 64),), -0.2, 0.2)), 0.2, 2.0),
        "misfit": normal_values(keys[5], (OBS, FIELDS), 4.0, 24.0, ((0, 64),), jnp.float32),
        "base_fields": normal_values(keys[6], (FIELDS, NZ, NX, NY), 1.0, 6.0, ((1, 64), (2, 8))),
    }


STORAGE = 0.05

def sweep_weights(count):
    order = []
    low, high = (0, count - 1)
    while low <= high:
        order.append(low)
        if high != low:
            order.append(high)
        low += 1
        high -= 1
    return [1.0 / (1.15 + 0.85 * math.cos((2 * i + 1) * math.pi / (2 * count))) for i in order]

def coefficients(cond_ext):
    padded = jnp.pad(cond_ext, ((0, 0), (1, 1), (1, 1)), mode='edge')
    centre = padded[1:-1, 1:-1, 1:-1]

    def harmonic(other):
        return 2.0 * centre * other / (centre + other)
    lower = harmonic(padded[:-2, 1:-1, 1:-1])
    upper = harmonic(padded[2:, 1:-1, 1:-1])
    west = harmonic(padded[1:-1, :-2, 1:-1])
    east = harmonic(padded[1:-1, 2:, 1:-1])
    south = harmonic(padded[1:-1, 1:-1, :-2])
    north = harmonic(padded[1:-1, 1:-1, 2:])
    diag = STORAGE + lower + upper + west + east + south + north
    return (lower, upper, west, east, south, north, diag)

def relax(u_ext, source, coeffs, weight):
    lower, upper, west, east, south, north, diag = coeffs
    core = u_ext[:, 1:-1]
    px = jnp.pad(core, ((0, 0), (0, 0), (1, 1), (0, 0)))
    py = jnp.pad(core, ((0, 0), (0, 0), (0, 0), (1, 1)))
    beside = lower * u_ext[:, :-2] + upper * u_ext[:, 2:] + west * px[:, :, :-2] + east * px[:, :, 2:] + south * py[..., :-2] + north * py[..., 2:]
    return core + weight * (source - (diag * core - beside)) / diag

def reference(log_cond, head_slope, modes, obs_cells, obs_var, misfit, base_fields):
    cond = jnp.exp(log_cond)
    coeffs = coefficients(jnp.pad(cond, ((1, 1), (0, 0), (0, 0)), mode='edge'))
    weights = sweep_weights(ITERS)
    positions = jnp.arange(OBS, dtype=jnp.int32) // OBS_SLAB * (CZ * NX * NY) + obs_cells.astype(jnp.int32)

    def respond(mode):
        source = (head_slope * cond * mode.astype(jnp.float32))[None]
        head = jnp.zeros_like(source)
        for weight in weights:
            head = relax(jnp.pad(head, ((0, 0), (1, 1), (0, 0), (0, 0))), source, coeffs, weight)
        return jnp.take(head.reshape(-1), positions)
    response = lax.map(respond, modes)
    scaled = response / obs_var[None, :]
    gram = jnp.dot(scaled, response.T, precision=lax.Precision.HIGHEST) + jnp.eye(response.shape[0], dtype=jnp.float32)
    rhs = jnp.dot(scaled, misfit, precision=lax.Precision.HIGHEST)
    factor = jnp.linalg.cholesky(gram)
    coef = jax.scipy.linalg.cho_solve((factor, True), rhs)

    def plane(level):
        layer = lax.dynamic_index_in_dim(modes, level, 1, keepdims=False)
        layer = layer.reshape(layer.shape[0], -1).astype(jnp.float32)
        return jnp.dot(coef.T, layer, precision=lax.Precision.HIGHEST).reshape(coef.shape[1], NX, NY)
    update = lax.map(plane, jnp.arange(NZ, dtype=jnp.int32))
    return base_fields.astype(jnp.float32) + jnp.transpose(update, (1, 0, 2, 3))
```

```python
import math

import jax
import jax.numpy as jnp
from jax import lax
from jax.experimental import pallas as pl
from jax.experimental.pallas import tpu as pltpu
from jax.sharding import Mesh
from jax.sharding import PartitionSpec as P

ITERS = 3
SLAB = ("slab_0", "slab_1")
MODE = ("mode_0", "mode_1")
STORAGE = 0.05
CZ = 4
NX = 128
NY = 128
LM = 8
OBS = 1024
MODES = 64
FIELDS = 16
ROWS = NX + 2
HI = lax.Precision.HIGHEST


def sweep_weights(count):
    order = []
    low, high = (0, count - 1)
    while low <= high:
        order.append(low)
        if high != low:
            order.append(high)
        low += 1
        high -= 1
    return [1.0 / (1.15 + 0.85 * math.cos((2 * i + 1) * math.pi / (2 * count))) for i in order]


W1, W2, W3 = sweep_weights(ITERS)


def harmonic(a, b):
    return 2.0 * a * b / (a + b)


def respond_kernel(edge, pick, lc, hs, before, after, modes, mbefore, mafter, out, coef, u1, u2, u3):
    first = edge[0] == 0
    last = edge[1] == 0
    rows = lax.broadcasted_iota(jnp.int32, (NX, NY), 0)
    cols = lax.broadcasted_iota(jnp.int32, (NX, NY), 1)

    own = [jnp.exp(lc[z]) for z in range(CZ)]
    cond = [jnp.where(first, own[0], jnp.exp(before[z])) for z in range(3)]
    cond += own
    cond += [jnp.where(last, own[CZ - 1], jnp.exp(after[z])) for z in range(3)]
    slope = [before[3], before[4]] + [hs[z] for z in range(CZ)] + [after[3], after[4]]
    faces = [harmonic(cond[z], cond[z + 1]) for z in range(9)]
    zero = jnp.zeros((LM, NY), jnp.float32)

    for e in range(8):
        c = cond[e + 1]
        lower = faces[e]
        upper = faces[e + 1]
        toward_e = jnp.where(rows == NX - 1, c, pltpu.roll(c, NX - 1, 0))
        east = harmonic(c, toward_e)
        west = jnp.where(rows == 0, harmonic(c, c), pltpu.roll(east, 1, 0))
        toward_n = jnp.where(cols == NY - 1, c, pltpu.roll(c, NY - 1, 1))
        north = harmonic(c, toward_n)
        south = jnp.where(cols == 0, harmonic(c, c), pltpu.roll(north, 1, 1))
        diag = STORAGE + lower + upper + west + east + south + north
        inv = 1.0 / diag
        if 1 <= e <= 6:
            keep = 1.0
            if e == 1:
                keep = jnp.where(first, 0.0, 1.0)
            if e == 6:
                keep = jnp.where(last, 0.0, 1.0)
            scale = inv * (W2 * keep)
            coef[0, e] = lower * scale
            coef[1, e] = upper * scale
            coef[2, e] = jnp.where(rows == 0, 0.0, west * scale)
            coef[3, e] = jnp.where(rows == NX - 1, 0.0, east * scale)
            coef[4, e] = jnp.where(cols == 0, 0.0, south * scale)
            coef[5, e] = jnp.where(cols == NY - 1, 0.0, north * scale)
        lead = slope[e] * c * inv * W1
        base = e * ROWS * LM
        u1[pl.ds(base, LM), :] = zero
        u1[pl.ds(base + (ROWS - 1) * LM, LM), :] = zero
        for k in range(LM):
            if e < 2:
                m = mbefore[k, e]
            elif e < 2 + CZ:
                m = modes[k, e - 2]
            else:
                m = mafter[k, e - 2 - CZ]
            u1[pl.ds(base + LM + k, NX, stride=LM), :] = m.astype(jnp.float32) * lead

    def at(ref, e, x):
        return ref[pl.ds(pl.multiple_of((e * ROWS + x) * LM, LM), LM), :]

    def sweep(ref, e, x):
        def c(i):
            return coef[i, e, pl.ds(x - 1, 1), :]

        u = at(ref, e, x)
        total = c(0) * at(ref, e - 1, x) + c(1) * at(ref, e + 1, x)
        total = total + (c(2) * at(ref, e, x - 1) + c(3) * at(ref, e, x + 1))
        total = total + (c(4) * pltpu.roll(u, 1, 1) + c(5) * pltpu.roll(u, NY - 1, 1))
        return u, total

    UN = 8
    for e in range(1, 7):
        base = e * ROWS * LM
        u2[pl.ds(base, LM), :] = zero
        u2[pl.ds(base + (ROWS - 1) * LM, LM), :] = zero
        own_weight = 1.0 - W2 + W2 / W1
        if e == 1:
            own_weight = jnp.where(first, 0.0, own_weight)
        if e == 6:
            own_weight = jnp.where(last, 0.0, own_weight)

        def second(i, _, e=e, own_weight=own_weight):
            for j in range(UN):
                x = i * UN + j + 1
                u, total = sweep(u1, e, x)
                u2[pl.ds(pl.multiple_of((e * ROWS + x) * LM, LM), LM), :] = own_weight * u + total
            return 0

        lax.fori_loop(0, NX // UN, second, 0)

    for e in range(2, 6):

        def third(i, _, e=e):
            for j in range(UN):
                x = i * UN + j + 1
                u, total = sweep(u2, e, x)
                value = (1.0 - W3) * u + (W3 / W1) * at(u1, e, x) + (W3 / W2) * total
                u3[(e - 2) * NX + x - 1] = value
            return 0

        lax.fori_loop(0, NX // UN, third, 0)

    lanes = lax.broadcasted_iota(jnp.int32, (LM, NY), 1)
    PU = 16

    def block(b, _):
        def group(g, acc):
            for j in range(PU):
                p = pick[b * NY + g * PU + j]
                row = u3[lax.shift_right_logical(p, 7)]
                acc = jnp.where(lanes == g * PU + j, pltpu.roll(row, p & 127, 1), acc)
            return acc

        got = lax.fori_loop(0, NY // PU, group, zero)
        for d in range(8):
            out[d, b] = got
        return 0

    lax.fori_loop(0, OBS // NY, block, 0)


def gram_kernel(resp, var, misfit, out):
    r = resp[...]
    scaled = r / var[...]
    mis = misfit[...]
    half = MODES // 2
    none = jnp.zeros((half, OBS), jnp.float32)
    none_f = jnp.zeros((FIELDS, OBS), jnp.float32)
    right_a = jnp.concatenate([r, none, mis, none_f], axis=0)
    right_b = jnp.concatenate([none, none, r[half:], none_f, mis], axis=0)
    dims = (((1,), (1,)), ((), ()))
    got = lax.dot_general(scaled[:half], right_a, dims, precision=HI, preferred_element_type=jnp.float32)
    got = got + lax.dot_general(
        scaled[half:], right_b, dims, precision=HI, preferred_element_type=jnp.float32
    )
    for d in range(8):
        out[d] = got


def total_kernel(parts, out):
    got = parts[0]
    for d in range(1, 8):
        got = got + parts[d]
    for d in range(8):
        out[d] = got


def solve_kernel(parts, out):
    p = parts[0]
    for d in range(1, 8):
        p = p + parts[d]
    half = MODES // 2
    lane = lax.broadcasted_iota(jnp.int32, (half, 128), 1)
    square = jnp.concatenate([p, jnp.zeros((128 - half, 128), jnp.float32)], axis=0)
    turned = square.T[half : 2 * half]
    near = pltpu.roll(p, 128 - 32, 1)
    far = pltpu.roll(p, 128 - 48, 1)
    top = jnp.where(lane < 64, p, near)
    low = jnp.where(lane < 32, turned, jnp.where(lane < 64, near, far))
    a = jnp.concatenate([top, low], axis=0)
    row = lax.broadcasted_iota(jnp.int32, (MODES, 128), 0)
    col = lax.broadcasted_iota(jnp.int32, (MODES, 128), 1)
    a = jnp.where(row == col, a + 1.0, a)
    a = [a[8 * i : 8 * i + 8] for i in range(8)]
    sub = lax.broadcasted_iota(jnp.int32, (8, 128), 0)

    def wide(v):
        return jnp.broadcast_to(v, (8, 128))

    for q in range(8):
        cs = [[wide(a[i][:, 8 * q + t : 8 * q + t + 1]) for i in range(8)] for t in range(8)]
        for t in range(8):
            c = cs[t]
            inv = 1.0 / wide(c[q][t : t + 1])
            norm = wide(a[q][t : t + 1]) * inv
            for i in range(8):
                new = a[i] - c[i] * norm
                a[i] = jnp.where(sub == t, norm, new) if i == q else new
            for s in range(t + 1, 8):
                f = wide(c[q][s : s + 1]) * inv
                for i in range(8):
                    new = cs[s][i] - c[i] * f
                    cs[s][i] = jnp.where(sub == t, f, new) if i == q else new
    for i in range(8):
        out[8 * i : 8 * i + 8, :] = a[i]


def vmem(n):
    return [pl.BlockSpec(memory_space=pltpu.VMEM)] * n


def smem(n):
    return [pl.BlockSpec(memory_space=pltpu.SMEM)] * n


def on_device(log_cond, head_slope, modes, obs_cells, obs_var, misfit, base_fields):
    slabs = lax.axis_size(SLAB)
    slab = lax.axis_index(SLAB)
    ahead = [(i, i + 1) for i in range(slabs - 1)]
    back = [(i + 1, i) for i in range(slabs - 1)]

    mbefore = lax.ppermute(modes[:, 2:4], SLAB, ahead)
    mafter = lax.ppermute(modes[:, 0:2], SLAB, back)
    before = lax.ppermute(jnp.concatenate([log_cond[1:4], head_slope[2:4]]), SLAB, ahead)
    after = lax.ppermute(jnp.concatenate([log_cond[0:3], head_slope[0:2]]), SLAB, back)

    pieces = jnp.moveaxis(modes.reshape(LM, CZ, 8, NX // 8, NY), 2, 0)
    block = lax.all_to_all(pieces, MODE, 0, 0, tiled=True)
    block, mbefore, mafter = lax.optimization_barrier((block, mbefore, mafter))

    edge = jnp.stack([slab, slabs - 1 - slab]).astype(jnp.int32)
    place = jnp.arange(OBS, dtype=jnp.int32)
    pick = (obs_cells & ~127) | ((place - obs_cells) & 127)
    copies = pl.pallas_call(
        respond_kernel,
        out_shape=jax.ShapeDtypeStruct((8, 8, LM, NY), jnp.float32),
        in_specs=smem(2) + vmem(7),
        out_specs=pl.BlockSpec(memory_space=pltpu.VMEM),
        scratch_shapes=[
            pltpu.VMEM((6, 8, NX, NY), jnp.float32),
            pltpu.VMEM((8 * ROWS * LM, NY), jnp.float32),
            pltpu.VMEM((8 * ROWS * LM, NY), jnp.float32),
            pltpu.VMEM((CZ * NX, LM, NY), jnp.float32),
        ],
        name="respond",
    )(edge, pick, log_cond, head_slope, before, after, modes, mbefore, mafter)
    whole = lax.all_to_all(copies, MODE, 0, 0, tiled=True)
    whole = jnp.moveaxis(whole, 1, 2).reshape(MODES, OBS)

    shared = jax.ShapeDtypeStruct((8, 32, 128), jnp.float32)
    part = pl.pallas_call(gram_kernel, out_shape=shared, in_specs=vmem(3), out_specs=vmem(1)[0], name="gram")(
        whole, obs_var.reshape(1, OBS), misfit.T
    )
    part = lax.all_to_all(part, "slab_1", 0, 0, tiled=True)
    part = pl.pallas_call(total_kernel, out_shape=shared, in_specs=vmem(1), out_specs=vmem(1)[0], name="total")(part)
    part = lax.all_to_all(part, "slab_0", 0, 0, tiled=True)
    solved = pl.pallas_call(
        solve_kernel,
        out_shape=jax.ShapeDtypeStruct((MODES, 128), jnp.float32),
        in_specs=vmem(1),
        out_specs=vmem(1)[0],
        name="solve",
    )(part)
    coef = solved[:, MODES : MODES + FIELDS]

    layer = block.reshape(MODES, CZ, NX // 8, NY).astype(jnp.float32)
    update = lax.dot_general(coef, layer, (((0,), (0,)), ((), ())), precision=HI)
    return base_fields.astype(jnp.float32) + update


def solution(mesh):
    torus = Mesh(mesh.devices.reshape(4, 2, 8, 8), ("mode_0", "mode_1", "slab_0", "slab_1"))
    in_specs = (
        P(SLAB, None, None),
        P(SLAB, None, None),
        P(MODE, SLAB, None, None),
        P(SLAB),
        P(SLAB),
        P(SLAB, None),
        P(None, SLAB, MODE, None),
    )
    out_specs = P(None, SLAB, MODE, None)
    return jax.shard_map(
        on_device, mesh=torus, in_specs=in_specs, out_specs=out_specs, check_vma=False
    )
```

```python
import functools
import math

import jax
import jax.numpy as jnp
from jax import lax
from jax.experimental import pallas as pl
from jax.experimental.pallas import tpu as pltpu
from jax.sharding import Mesh
from jax.sharding import PartitionSpec as P

ITERS = 3
SLAB = ("slab_0", "slab_1")
MODE = ("mode_0", "mode_1")
STORAGE = 0.05
CZ = 4
NX = 128
NY = 128
LM = 8
OBS = 1024
MODES = 64
FIELDS = 16
ROWS = NX + 2
HI = lax.Precision.HIGHEST


def sweep_weights(count):
    order = []
    low, high = (0, count - 1)
    while low <= high:
        order.append(low)
        if high != low:
            order.append(high)
        low += 1
        high -= 1
    return [1.0 / (1.15 + 0.85 * math.cos((2 * i + 1) * math.pi / (2 * count))) for i in order]


W1, W2, W3 = sweep_weights(ITERS)
OWN2 = 1.0 - W2 + W2 / W1


def harmonic(a, b):
    return 2.0 * a * b / (a + b)


def at(ref, e, x):
    return ref[pl.ds(pl.multiple_of((e * ROWS + x) * LM, LM), LM), :]


def put(ref, e, x, value):
    ref[pl.ds(pl.multiple_of((e * ROWS + x) * LM, LM), LM), :] = value


def sweep(coef, ref, e, x):
    def c(i):
        return coef[i, e, pl.ds(x - 1, 1), :]

    u = at(ref, e, x)
    total = c(0) * at(ref, e - 1, x) + c(1) * at(ref, e + 1, x)
    total = total + (c(2) * at(ref, e, x - 1) + c(3) * at(ref, e, x + 1))
    total = total + (c(4) * pltpu.roll(u, 1, 1) + c(5) * pltpu.roll(u, NY - 1, 1))
    return u, total


def over_rows(planes, unroll, fn):
    first, step, count = planes
    pieces = NX // unroll

    def body(i, _):
        e = first + step * (i // pieces)
        start = (i % pieces) * unroll + 1
        for j in range(unroll):
            fn(e, start + j)
        return 0

    lax.fori_loop(0, count * pieces, body, 0)


def second_row(coef, u1, u2, e, x):
    u, total = sweep(coef, u1, e, x)
    put(u2, e, x, OWN2 * u + total)


def pick_block(pick, u3, first, out, slot):
    lanes = lax.broadcasted_iota(jnp.int32, (LM, NY), 1)
    acc = jnp.zeros((LM, NY), jnp.float32)
    for j in range(NY):
        p = pick[first + j]
        row = u3[lax.shift_right_logical(p, 7)]
        acc = jnp.where(lanes == j, pltpu.roll(row, p & 127, 1), acc)
    out[slot] = acc


def clear_edges(ref, e):
    zero = jnp.zeros((LM, NY), jnp.float32)
    put(ref, e, 0, zero)
    put(ref, e, ROWS - 1, zero)


def outer_kernel(edge, pick, lc, hs, before, after, modes, share, coef, u1, u2, u3):
    first = edge[0] == 0
    last = edge[1] == 0
    rows = lax.broadcasted_iota(jnp.int32, (NX, NY), 0)
    cols = lax.broadcasted_iota(jnp.int32, (NX, NY), 1)
    zero = jnp.zeros((LM, NY), jnp.float32)

    own = [jnp.exp(lc[z]) for z in range(CZ)]
    cond = [jnp.where(first, own[0], jnp.exp(before[NX * z : NX * z + NX])) for z in range(3)]
    cond += own
    cond += [jnp.where(last, own[CZ - 1], jnp.exp(after[NX * z : NX * z + NX])) for z in range(3)]
    faces = [harmonic(cond[z], cond[z + 1]) for z in range(9)]

    for e in range(8):
        c = cond[e + 1]
        lower = faces[e]
        upper = faces[e + 1]
        toward_e = jnp.where(rows == NX - 1, c, pltpu.roll(c, NX - 1, 0))
        east = harmonic(c, toward_e)
        west = jnp.where(rows == 0, harmonic(c, c), pltpu.roll(east, 1, 0))
        toward_n = jnp.where(cols == NY - 1, c, pltpu.roll(c, NY - 1, 1))
        north = harmonic(c, toward_n)
        south = jnp.where(cols == 0, harmonic(c, c), pltpu.roll(north, 1, 1))
        diag = STORAGE + lower + upper + west + east + south + north
        inv = 1.0 / diag
        scale = inv * W2
        if e == 1:
            scale = jnp.where(first, 0.0, scale)
        if e == 6:
            scale = jnp.where(last, 0.0, scale)
        coef[0, e] = lower * scale
        coef[1, e] = upper * scale
        if 1 <= e <= 6:
            coef[2, e] = jnp.where(rows == 0, 0.0, west * scale)
            coef[3, e] = jnp.where(rows == NX - 1, 0.0, east * scale)
            coef[4, e] = jnp.where(cols == 0, 0.0, south * scale)
            coef[5, e] = jnp.where(cols == NY - 1, 0.0, north * scale)
            clear_edges(u2, e)
        if 2 <= e <= 5:
            clear_edges(u1, e)
            lead = hs[e - 2] * c * inv * W1
            for k in range(LM):
                m = modes[k, e - 2].astype(jnp.float32)
                u1[pl.ds((e * ROWS + 1) * LM + k, NX, stride=LM), :] = m * lead

    def clear(i, _):
        for j in range(13):
            x = i * 13 + j
            put(u1, 1, x, zero)
            put(u1, 6, x, zero)
            put(u2, 0, x, zero)
            put(u2, 7, x, zero)
        return 0

    lax.fori_loop(0, ROWS // 13, clear, 0)
    for j in range(8):
        u3[8 * NX + j] = zero

    def c(i, e, x):
        return coef[i, e, pl.ds(x - 1, 1), :]

    def end_two(e, x):
        put(u2, 1, x, c(1, 1, x) * at(u1, 2, x))
        put(u2, 6, x, c(0, 6, x) * at(u1, 5, x))

    over_rows((0, 0, 1), 16, end_two)
    over_rows((2, 3, 2), 64, functools.partial(second_row, coef, u1, u2))

    def end_three(e, x):
        u3[x - 1] = (W3 / W2) * (c(1, 0, x) * at(u2, 1, x))
        u3[7 * NX + x - 1] = (W3 / W2) * (c(0, 7, x) * at(u2, 6, x))

    over_rows((0, 0, 1), 16, end_three)

    def third(e, x):
        u, total = sweep(coef, u2, e, x)
        u3[e * NX + x - 1] = (1.0 - W3) * u + (W3 / W2) * total

    over_rows((1, 5, 2), 64, third)

    def block(b, _):
        pick_block(pick, u3, b * NY, share, b)
        return 0

    lax.fori_loop(0, 16, block, 0)


def inner_kernel(pick, coef, u1, u2, out, w2, u3):
    def second(e, x):
        u, total = sweep(coef, u1, e, x)
        put(w2, e - 2, x, OWN2 * u + total)

    clear_edges(w2, 1)
    clear_edges(w2, 2)
    over_rows((3, 1, 2), 64, second)

    def third(e, x, here, below, above):
        def c(i):
            return coef[i, e, pl.ds(x - 1, 1), :]

        u = here(x)
        total = c(0) * below(x) + c(1) * above(x)
        total = total + (c(2) * here(x - 1) + c(3) * here(x + 1))
        total = total + (c(4) * pltpu.roll(u, 1, 1) + c(5) * pltpu.roll(u, NY - 1, 1))
        value = (1.0 - W3) * u + (W3 / W1) * at(u1, e, x) + (W3 / W2) * total
        u3[(e - 2) * NX + x - 1] = value

    def plane(ref, e):
        return lambda x: at(ref, e, x)

    lines = {e: plane(u2, e) for e in (1, 2, 5, 6)}
    lines.update({e: plane(w2, e - 2) for e in (3, 4)})
    for q in range(4):
        over_rows(
            (q + 2, 0, 1),
            64,
            lambda e, x, q=q: third(q + 2, x, lines[q + 2], lines[q + 1], lines[q + 3]),
        )

    def block(b, _):
        pick_block(pick, u3, b * NY, out, b)
        return 0

    lax.fori_loop(0, 8, block, 0)


def gram_kernel(resp, var, misfit, out):
    r = resp[...]
    scaled = r / var[...]
    mis = misfit[...]
    half = MODES // 2
    none = jnp.zeros((half, OBS), jnp.float32)
    none_f = jnp.zeros((FIELDS, OBS), jnp.float32)
    right_a = jnp.concatenate([r, none, mis, none_f], axis=0)
    right_b = jnp.concatenate([none, none, r[half:], none_f, mis], axis=0)
    dims = (((1,), (1,)), ((), ()))
    got = lax.dot_general(scaled[:half], right_a, dims, precision=HI, preferred_element_type=jnp.float32)
    got = got + lax.dot_general(
        scaled[half:], right_b, dims, precision=HI, preferred_element_type=jnp.float32
    )
    for d in range(8):
        out[d] = got


def total_kernel(parts, out):
    got = parts[0]
    for d in range(1, 8):
        got = got + parts[d]
    for d in range(8):
        out[d] = got


def solve_kernel(parts, out):
    p = parts[0]
    for d in range(1, 8):
        p = p + parts[d]
    half = MODES // 2
    lane = lax.broadcasted_iota(jnp.int32, (half, 128), 1)
    square = jnp.concatenate([p, jnp.zeros((128 - half, 128), jnp.float32)], axis=0)
    turned = square.T[half : 2 * half]
    near = pltpu.roll(p, 128 - 32, 1)
    far = pltpu.roll(p, 128 - 48, 1)
    top = jnp.where(lane < 64, p, near)
    low = jnp.where(lane < 32, turned, jnp.where(lane < 64, near, far))
    a = jnp.concatenate([top, low], axis=0)
    row = lax.broadcasted_iota(jnp.int32, (MODES, 128), 0)
    col = lax.broadcasted_iota(jnp.int32, (MODES, 128), 1)
    a = jnp.where(row == col, a + 1.0, a)
    a = [a[8 * i : 8 * i + 8] for i in range(8)]
    sub = lax.broadcasted_iota(jnp.int32, (8, 128), 0)

    def wide(v):
        return jnp.broadcast_to(v, (8, 128))

    for q in range(8):
        cs = [[wide(a[i][:, 8 * q + t : 8 * q + t + 1]) for i in range(8)] for t in range(8)]
        for t in range(8):
            c = cs[t]
            inv = 1.0 / wide(c[q][t : t + 1])
            norm = wide(a[q][t : t + 1]) * inv
            for i in range(8):
                new = a[i] - c[i] * norm
                a[i] = jnp.where(sub == t, norm, new) if i == q else new
            for s in range(t + 1, 8):
                f = wide(c[q][s : s + 1]) * inv
                for i in range(8):
                    new = cs[s][i] - c[i] * f
                    cs[s][i] = jnp.where(sub == t, f, new) if i == q else new
    for i in range(8):
        out[8 * i : 8 * i + 8, :] = a[i]


def vmem(n):
    return [pl.BlockSpec(memory_space=pltpu.VMEM)] * n


def smem(n):
    return [pl.BlockSpec(memory_space=pltpu.SMEM)] * n


def limit(mib):
    return pltpu.CompilerParams(vmem_limit_bytes=mib * 1024 * 1024)


def on_device(log_cond, head_slope, modes, obs_cells, obs_var, misfit, base_fields):
    slabs = lax.axis_size(SLAB)
    slab = lax.axis_index(SLAB)
    ahead = [(i, i + 1) for i in range(slabs - 1)]
    back = [(i + 1, i) for i in range(slabs - 1)]

    cells = obs_cells.astype(jnp.float32).reshape(8, NY)
    upward = jnp.concatenate([log_cond[1:4].reshape(3 * NX, NY), cells])
    downward = jnp.concatenate([log_cond[0:3].reshape(3 * NX, NY), cells])
    before = lax.ppermute(upward, SLAB, ahead)
    after = lax.ppermute(downward, SLAB, back)

    pieces = jnp.moveaxis(modes.reshape(LM, CZ, 8, NX // 8, NY), 2, 0)
    block = lax.all_to_all(pieces, MODE, 0, 0, tiled=True)

    edge = jnp.stack([slab, slabs - 1 - slab]).astype(jnp.int32)
    place = jnp.arange(OBS, dtype=jnp.int32)

    def address(where, shift, low, high):
        plane = where >> 14
        row = jnp.where((plane >= low) & (plane <= high), (where >> 7) + shift * NX, 8 * NX)
        return (row << 7) | ((place - where) & 127)

    def arrived(x):
        return x[3 * NX :].astype(jnp.int32).reshape(OBS)

    far_pick = jnp.concatenate([address(arrived(before), -2, 2, 3), address(arrived(after), 6, 0, 1)])
    near_pick = address(obs_cells, 0, 0, 3)
    plane_rows = jax.ShapeDtypeStruct((8 * ROWS * LM, NY), jnp.float32)
    share, coefs, u1, u2 = pl.pallas_call(
        outer_kernel,
        out_shape=(
            jax.ShapeDtypeStruct((16, LM, NY), jnp.float32),
            jax.ShapeDtypeStruct((6, 8, NX, NY), jnp.float32),
            plane_rows,
            plane_rows,
        ),
        in_specs=smem(2) + vmem(5),
        out_specs=vmem(4),
        scratch_shapes=[pltpu.VMEM((8 * NX + 8, LM, NY), jnp.float32)],
        compiler_params=limit(24),
        name="outer",
    )(edge, far_pick, log_cond, head_slope, before, after, modes)
    from_above = lax.ppermute(share[:8], SLAB, back)
    from_below = lax.ppermute(share[8:], SLAB, ahead)
    picked = pl.pallas_call(
        inner_kernel,
        out_shape=jax.ShapeDtypeStruct((8, LM, NY), jnp.float32),
        in_specs=smem(1) + vmem(3),
        out_specs=vmem(1)[0],
        scratch_shapes=[
            pltpu.VMEM((4 * ROWS * LM, NY), jnp.float32),
            pltpu.VMEM((4 * NX + 8, LM, NY), jnp.float32),
        ],
        compiler_params=limit(24),
        name="inner",
    )(near_pick, coefs, u1, u2)
    block, from_above, from_below = lax.optimization_barrier((block, from_above, from_below))
    picked = picked + from_above + from_below
    copies = jnp.broadcast_to(picked, (8, 8, LM, NY))
    whole = lax.all_to_all(copies, MODE, 0, 0, tiled=True)
    whole = jnp.moveaxis(whole, 1, 2).reshape(MODES, OBS)

    shared = jax.ShapeDtypeStruct((8, 32, 128), jnp.float32)
    part = pl.pallas_call(gram_kernel, out_shape=shared, in_specs=vmem(3), out_specs=vmem(1)[0], compiler_params=limit(6), name="gram")(
        whole, obs_var.reshape(1, OBS), misfit.T
    )
    part = lax.all_to_all(part, "slab_1", 0, 0, tiled=True)
    part = pl.pallas_call(total_kernel, out_shape=shared, in_specs=vmem(1), out_specs=vmem(1)[0], compiler_params=limit(4), name="total")(part)
    part = lax.all_to_all(part, "slab_0", 0, 0, tiled=True)
    solved = pl.pallas_call(
        solve_kernel,
        out_shape=jax.ShapeDtypeStruct((MODES, 128), jnp.float32),
        in_specs=vmem(1),
        out_specs=vmem(1)[0],
        compiler_params=limit(4),
        name="solve",
    )(part)
    coef = solved[:, MODES : MODES + FIELDS]

    layer = block.reshape(MODES, CZ, NX // 8, NY).astype(jnp.float32)
    update = lax.dot_general(coef, layer, (((0,), (0,)), ((), ())), precision=HI)
    return base_fields.astype(jnp.float32) + update


def solution(mesh):
    torus = Mesh(mesh.devices.reshape(4, 2, 8, 8), ("mode_0", "mode_1", "slab_0", "slab_1"))
    in_specs = (
        P(SLAB, None, None),
        P(SLAB, None, None),
        P(MODE, SLAB, None, None),
        P(SLAB),
        P(SLAB),
        P(SLAB, None),
        P(None, SLAB, MODE, None),
    )
    out_specs = P(None, SLAB, MODE, None)
    return jax.shard_map(
        on_device, mesh=torus, in_specs=in_specs, out_specs=out_specs, check_vma=False
    )
```

```python
import functools
import math

import jax
import jax.numpy as jnp
from jax import lax
from jax.experimental import pallas as pl
from jax.experimental.pallas import tpu as pltpu
from jax.sharding import Mesh
from jax.sharding import PartitionSpec as P

ITERS = 3
SLAB = ("slab_0", "slab_1")
MODE = ("mode_0", "mode_1")
STORAGE = 0.05
CZ = 4
NX = 128
NY = 128
LM = 8
OBS = 1024
MODES = 64
FIELDS = 16
ROWS = NX + 2
HI = lax.Precision.HIGHEST


def sweep_weights(count):
    order = []
    low, high = (0, count - 1)
    while low <= high:
        order.append(low)
        if high != low:
            order.append(high)
        low += 1
        high -= 1
    return [1.0 / (1.15 + 0.85 * math.cos((2 * i + 1) * math.pi / (2 * count))) for i in order]


W1, W2, W3 = sweep_weights(ITERS)
OWN2 = 1.0 - W2 + W2 / W1


def harmonic(a, b):
    return 2.0 * a * b / (a + b)


def at(ref, e, x):
    return ref[pl.ds(pl.multiple_of((e * ROWS + x) * LM, LM), LM), :]


def put(ref, e, x, value):
    ref[pl.ds(pl.multiple_of((e * ROWS + x) * LM, LM), LM), :] = value


def sweep(coef, ref, e, x):
    def c(i):
        return coef[i, e, pl.ds(x - 1, 1), :]

    u = at(ref, e, x)
    total = c(0) * at(ref, e - 1, x) + c(1) * at(ref, e + 1, x)
    total = total + (c(2) * at(ref, e, x - 1) + c(3) * at(ref, e, x + 1))
    total = total + (c(4) * pltpu.roll(u, 1, 1) + c(5) * pltpu.roll(u, NY - 1, 1))
    return u, total


def over_rows(planes, unroll, fn):
    first, step, count = planes
    pieces = NX // unroll

    def body(i, _):
        e = first + step * (i // pieces)
        start = (i % pieces) * unroll + 1
        for j in range(unroll):
            fn(e, start + j)
        return 0

    lax.fori_loop(0, count * pieces, body, 0)


def second_row(coef, u1, u2, e, x):
    u, total = sweep(coef, u1, e, x)
    put(u2, e, x, OWN2 * u + total)


def pick_block(pick, u3, b, out):
    lanes = lax.broadcasted_iota(jnp.int32, (LM, NY), 1)
    acc = jnp.zeros((LM, NY), jnp.float32)
    for j in range(NY):
        p = pick[b, j]
        row = u3[pl.ds(pl.multiple_of(lax.shift_right_logical(p, 7), LM), LM), :]
        acc = jnp.where(lanes == j, pltpu.roll(row, p & 127, 1), acc)
    out[b] = acc


def put_row(ref, row, value):
    ref[pl.ds(pl.multiple_of(row * LM, LM), LM), :] = value


def clear_edges(ref, e):
    zero = jnp.zeros((LM, NY), jnp.float32)
    put(ref, e, 0, zero)
    put(ref, e, ROWS - 1, zero)


def address(where, place, shift, low, high):
    plane = where >> 14
    row = jnp.where((plane >= low) & (plane <= high), (where >> 7) + shift * NX, 8 * NX)
    return (row << 10) | ((place - where) & 127)


def pack_kernel(lc, cells, upward, downward, near):
    for z in range(3):
        upward[NX * z : NX * z + NX] = lc[z + 1]
        downward[NX * z : NX * z + NX] = lc[z]
    where = cells[...]
    upward[3 * NX :] = where.astype(jnp.float32)
    downward[3 * NX :] = where.astype(jnp.float32)
    place = lax.broadcasted_iota(jnp.int32, (8, NY), 1)
    near[...] = address(where, place, 0, 0, 3)


def outer_kernel(edge, pick, lc, hs, before, after, modes, share, coef, u1, u2, u3):
    first = edge[0] == 0
    last = edge[1] == 0
    rows = lax.broadcasted_iota(jnp.int32, (NX, NY), 0)
    cols = lax.broadcasted_iota(jnp.int32, (NX, NY), 1)
    zero = jnp.zeros((LM, NY), jnp.float32)

    own = [jnp.exp(lc[z]) for z in range(CZ)]
    cond = [jnp.where(first, own[0], jnp.exp(before[NX * z : NX * z + NX])) for z in range(3)]
    cond += own
    cond += [jnp.where(last, own[CZ - 1], jnp.exp(after[NX * z : NX * z + NX])) for z in range(3)]
    faces = [harmonic(cond[z], cond[z + 1]) for z in range(9)]

    for e in range(8):
        c = cond[e + 1]
        lower = faces[e]
        upper = faces[e + 1]
        toward_e = jnp.where(rows == NX - 1, c, pltpu.roll(c, NX - 1, 0))
        east = harmonic(c, toward_e)
        west = jnp.where(rows == 0, c, pltpu.roll(east, 1, 0))
        toward_n = jnp.where(cols == NY - 1, c, pltpu.roll(c, NY - 1, 1))
        north = harmonic(c, toward_n)
        south = jnp.where(cols == 0, c, pltpu.roll(north, 1, 1))
        diag = STORAGE + lower + upper + west + east + south + north
        inv = 1.0 / diag
        scale = inv * W2
        if e == 1:
            scale = jnp.where(first, 0.0, scale)
        if e == 6:
            scale = jnp.where(last, 0.0, scale)
        coef[0, e] = lower * scale
        coef[1, e] = upper * scale
        if 1 <= e <= 6:
            coef[2, e] = jnp.where(rows == 0, 0.0, west * scale)
            coef[3, e] = jnp.where(rows == NX - 1, 0.0, east * scale)
            coef[4, e] = jnp.where(cols == 0, 0.0, south * scale)
            coef[5, e] = jnp.where(cols == NY - 1, 0.0, north * scale)
            clear_edges(u2, e)
        if 2 <= e <= 5:
            clear_edges(u1, e)
            lead = hs[e - 2] * c * inv * W1
            for k in range(LM):
                m = modes[k, e - 2].astype(jnp.float32)
                u1[pl.ds((e * ROWS + 1) * LM + k, NX, stride=LM), :] = m * lead

    def clear(i, _):
        for j in range(13):
            x = i * 13 + j
            put(u1, 1, x, zero)
            put(u1, 6, x, zero)
            put(u2, 0, x, zero)
            put(u2, 7, x, zero)
        return 0

    lax.fori_loop(0, ROWS // 13, clear, 0)
    for j in range(8):
        put_row(u3, 8 * NX + j, zero)

    def c(i, e, x):
        return coef[i, e, pl.ds(x - 1, 1), :]

    def end_two(e, x):
        put(u2, 1, x, c(1, 1, x) * at(u1, 2, x))
        put(u2, 6, x, c(0, 6, x) * at(u1, 5, x))

    over_rows((0, 0, 1), 16, end_two)
    over_rows((2, 3, 2), 64, functools.partial(second_row, coef, u1, u2))

    def end_three(e, x):
        put_row(u3, x - 1, (W3 / W2) * (c(1, 0, x) * at(u2, 1, x)))
        put_row(u3, 7 * NX + x - 1, (W3 / W2) * (c(0, 7, x) * at(u2, 6, x)))

    over_rows((0, 0, 1), 16, end_three)

    def third(e, x):
        u, total = sweep(coef, u2, e, x)
        put_row(u3, e * NX + x - 1, (1.0 - W3) * u + (W3 / W2) * total)

    over_rows((1, 5, 2), 64, third)

    def block(b, _):
        pick_block(pick, u3, b, share)
        return 0

    lax.fori_loop(0, 16, block, 0)


def inner_kernel(pick, coef, u1, u2, out, w2, u3):
    def second(e, x):
        u, total = sweep(coef, u1, e, x)
        put(w2, e - 2, x, OWN2 * u + total)

    clear_edges(w2, 1)
    clear_edges(w2, 2)
    over_rows((3, 1, 2), 64, second)

    def third(e, x, here, below, above):
        def c(i):
            return coef[i, e, pl.ds(x - 1, 1), :]

        u = here(x)
        total = c(0) * below(x) + c(1) * above(x)
        total = total + (c(2) * here(x - 1) + c(3) * here(x + 1))
        total = total + (c(4) * pltpu.roll(u, 1, 1) + c(5) * pltpu.roll(u, NY - 1, 1))
        value = (1.0 - W3) * u + (W3 / W1) * at(u1, e, x) + (W3 / W2) * total
        put_row(u3, (e - 2) * NX + x - 1, value)

    def plane(ref, e):
        return lambda x: at(ref, e, x)

    lines = {e: plane(u2, e) for e in (1, 2, 5, 6)}
    lines.update({e: plane(w2, e - 2) for e in (3, 4)})
    for q in range(4):
        over_rows(
            (q + 2, 0, 1),
            64,
            lambda e, x, q=q: third(q + 2, x, lines[q + 2], lines[q + 1], lines[q + 3]),
        )

    def block(b, _):
        pick_block(pick, u3, b, out)
        return 0

    lax.fori_loop(0, 8, block, 0)


def gram_kernel(resp, var, misfit, out):
    r = resp[...]
    scaled = r / var[...]
    mis = misfit[...]
    half = MODES // 2
    none = jnp.zeros((half, OBS), jnp.float32)
    none_f = jnp.zeros((FIELDS, OBS), jnp.float32)
    right_a = jnp.concatenate([r, none, mis, none_f], axis=0)
    right_b = jnp.concatenate([none, none, r[half:], none_f, mis], axis=0)
    dims = (((1,), (1,)), ((), ()))
    got = lax.dot_general(scaled[:half], right_a, dims, precision=HI, preferred_element_type=jnp.float32)
    got = got + lax.dot_general(
        scaled[half:], right_b, dims, precision=HI, preferred_element_type=jnp.float32
    )
    for d in range(8):
        out[d] = got


def total_kernel(parts, out):
    got = parts[0]
    for d in range(1, 8):
        got = got + parts[d]
    for d in range(8):
        out[d] = got


def solve_kernel(parts, out):
    p = parts[0]
    for d in range(1, 8):
        p = p + parts[d]
    half = MODES // 2
    lane = lax.broadcasted_iota(jnp.int32, (half, 128), 1)
    square = jnp.concatenate([p, jnp.zeros((128 - half, 128), jnp.float32)], axis=0)
    turned = square.T[half : 2 * half]
    near = pltpu.roll(p, 128 - 32, 1)
    far = pltpu.roll(p, 128 - 48, 1)
    top = jnp.where(lane < 64, p, near)
    low = jnp.where(lane < 32, turned, jnp.where(lane < 64, near, far))
    a = jnp.concatenate([top, low], axis=0)
    row = lax.broadcasted_iota(jnp.int32, (MODES, 128), 0)
    col = lax.broadcasted_iota(jnp.int32, (MODES, 128), 1)
    a = jnp.where(row == col, a + 1.0, a)
    a = [a[8 * i : 8 * i + 8] for i in range(8)]
    sub = lax.broadcasted_iota(jnp.int32, (8, 128), 0)

    def wide(v):
        return jnp.broadcast_to(v, (8, 128))

    for q in range(8):
        cs = [[wide(a[i][:, 8 * q + t : 8 * q + t + 1]) for i in range(8)] for t in range(8)]
        for t in range(8):
            c = cs[t]
            inv = 1.0 / wide(c[q][t : t + 1])
            norm = wide(a[q][t : t + 1]) * inv
            for i in range(8):
                new = a[i] - c[i] * norm
                a[i] = jnp.where(sub == t, norm, new) if i == q else new
            for s in range(t + 1, 8):
                f = wide(c[q][s : s + 1]) * inv
                for i in range(8):
                    new = cs[s][i] - c[i] * f
                    cs[s][i] = jnp.where(sub == t, f, new) if i == q else new
    for i in range(8):
        out[8 * i : 8 * i + 8, :] = a[i]


def vmem(n):
    return [pl.BlockSpec(memory_space=pltpu.VMEM)] * n


def smem(n):
    return [pl.BlockSpec(memory_space=pltpu.SMEM)] * n


def limit(mib):
    return pltpu.CompilerParams(vmem_limit_bytes=mib * 1024 * 1024)


def on_device(log_cond, head_slope, modes, obs_cells, obs_var, misfit, base_fields):
    slabs = lax.axis_size(SLAB)
    slab = lax.axis_index(SLAB)
    ahead = [(i, i + 1) for i in range(slabs - 1)]
    back = [(i + 1, i) for i in range(slabs - 1)]

    message = jax.ShapeDtypeStruct((3 * NX + 8, NY), jnp.float32)
    upward, downward, near_pick = pl.pallas_call(
        pack_kernel,
        out_shape=(message, message, jax.ShapeDtypeStruct((8, NY), jnp.int32)),
        in_specs=vmem(2),
        out_specs=vmem(3),
        compiler_params=limit(4),
        name="pack",
    )(log_cond, obs_cells.reshape(8, NY))
    before = lax.ppermute(upward, SLAB, ahead)
    after = lax.ppermute(downward, SLAB, back)

    pieces = jnp.moveaxis(modes.reshape(LM, CZ, 8, NX // 8, NY), 2, 0)
    block = lax.all_to_all(pieces, MODE, 0, 0, tiled=True)

    edge = jnp.stack([slab, slabs - 1 - slab]).astype(jnp.int32)
    place = lax.broadcasted_iota(jnp.int32, (8, NY), 1)

    def arrived(x):
        return x[3 * NX :].astype(jnp.int32)

    far_pick = jnp.concatenate(
        [address(arrived(before), place, -2, 2, 3), address(arrived(after), place, 6, 0, 1)]
    )
    plane_rows = jax.ShapeDtypeStruct((8 * ROWS * LM, NY), jnp.float32)
    share, coefs, u1, u2 = pl.pallas_call(
        outer_kernel,
        out_shape=(
            jax.ShapeDtypeStruct((16, LM, NY), jnp.float32),
            jax.ShapeDtypeStruct((6, 8, NX, NY), jnp.float32),
            plane_rows,
            plane_rows,
        ),
        in_specs=smem(2) + vmem(5),
        out_specs=vmem(4),
        scratch_shapes=[pltpu.VMEM(((8 * NX + 8) * LM, NY), jnp.float32)],
        compiler_params=limit(24),
        name="outer",
    )(edge, far_pick, log_cond, head_slope, before, after, modes)
    from_above = lax.ppermute(share[:8], SLAB, back)
    from_below = lax.ppermute(share[8:], SLAB, ahead)
    picked = pl.pallas_call(
        inner_kernel,
        out_shape=jax.ShapeDtypeStruct((8, LM, NY), jnp.float32),
        in_specs=smem(1) + vmem(3),
        out_specs=vmem(1)[0],
        scratch_shapes=[
            pltpu.VMEM((4 * ROWS * LM, NY), jnp.float32),
            pltpu.VMEM((4 * NX * LM, NY), jnp.float32),
        ],
        compiler_params=limit(24),
        name="inner",
    )(near_pick, coefs, u1, u2)
    block, from_above, from_below = lax.optimization_barrier((block, from_above, from_below))
    picked = picked + from_above + from_below
    copies = jnp.broadcast_to(picked, (8, 8, LM, NY))
    whole = lax.all_to_all(copies, MODE, 0, 0, tiled=True)
    whole = jnp.moveaxis(whole, 1, 2).reshape(MODES, OBS)

    shared = jax.ShapeDtypeStruct((8, 32, 128), jnp.float32)
    part = pl.pallas_call(gram_kernel, out_shape=shared, in_specs=vmem(3), out_specs=vmem(1)[0], compiler_params=limit(6), name="gram")(
        whole, obs_var.reshape(1, OBS), misfit.T
    )
    part = lax.all_to_all(part, "slab_1", 0, 0, tiled=True)
    part = pl.pallas_call(total_kernel, out_shape=shared, in_specs=vmem(1), out_specs=vmem(1)[0], compiler_params=limit(4), name="total")(part)
    part = lax.all_to_all(part, "slab_0", 0, 0, tiled=True)
    solved = pl.pallas_call(
        solve_kernel,
        out_shape=jax.ShapeDtypeStruct((MODES, 128), jnp.float32),
        in_specs=vmem(1),
        out_specs=vmem(1)[0],
        compiler_params=limit(4),
        name="solve",
    )(part)
    coef = solved[:, MODES : MODES + FIELDS]

    layer = block.reshape(MODES, CZ, NX // 8, NY).astype(jnp.float32)
    update = lax.dot_general(coef, layer, (((0,), (0,)), ((), ())), precision=HI)
    return base_fields.astype(jnp.float32) + update


def solution(mesh):
    torus = Mesh(mesh.devices.reshape(4, 2, 8, 8), ("mode_0", "mode_1", "slab_0", "slab_1"))
    in_specs = (
        P(SLAB, None, None),
        P(SLAB, None, None),
        P(MODE, SLAB, None, None),
        P(SLAB),
        P(SLAB),
        P(SLAB, None),
        P(None, SLAB, MODE, None),
    )
    out_specs = P(None, SLAB, MODE, None)
    return jax.shard_map(
        on_device, mesh=torus, in_specs=in_specs, out_specs=out_specs, check_vma=False
    )
```

```python
import functools
import math

import jax
import jax.numpy as jnp
from jax import lax
from jax.experimental import pallas as pl
from jax.experimental.pallas import tpu as pltpu
from jax.sharding import Mesh
from jax.sharding import PartitionSpec as P

ITERS = 3
SLAB = ("slab_0", "slab_1")
MODE = ("mode_0", "mode_1")
STORAGE = 0.05
CZ = 4
NX = 128
NY = 128
LM = 8
OBS = 1024
MODES = 64
FIELDS = 16
ROWS = NX + 2
HI = lax.Precision.HIGHEST


def sweep_weights(count):
    order = []
    low, high = (0, count - 1)
    while low <= high:
        order.append(low)
        if high != low:
            order.append(high)
        low += 1
        high -= 1
    return [1.0 / (1.15 + 0.85 * math.cos((2 * i + 1) * math.pi / (2 * count))) for i in order]


W1, W2, W3 = sweep_weights(ITERS)
OWN2 = 1.0 - W2 + W2 / W1


def harmonic(a, b):
    return 2.0 * a * b / (a + b)


def at(ref, e, x):
    return ref[pl.ds(pl.multiple_of((e * ROWS + x) * LM, LM), LM), :]


def put(ref, e, x, value):
    ref[pl.ds(pl.multiple_of((e * ROWS + x) * LM, LM), LM), :] = value


def sweep(coef, ref, e, x):
    def c(i):
        return coef[i, e, pl.ds(x - 1, 1), :]

    u = at(ref, e, x)
    total = c(0) * at(ref, e - 1, x) + c(1) * at(ref, e + 1, x)
    total = total + (c(2) * at(ref, e, x - 1) + c(3) * at(ref, e, x + 1))
    total = total + (c(4) * pltpu.roll(u, 1, 1) + c(5) * pltpu.roll(u, NY - 1, 1))
    return u, total


def over_rows(planes, unroll, fn):
    first, step, count = planes
    pieces = NX // unroll

    def body(i, _):
        e = first + step * (i // pieces)
        start = (i % pieces) * unroll + 1
        for j in range(unroll):
            fn(e, start + j)
        return 0

    lax.fori_loop(0, count * pieces, body, 0)


def second_row(coef, u1, u2, e, x):
    u, total = sweep(coef, u1, e, x)
    put(u2, e, x, OWN2 * u + total)


def pick_block(pick, u3, b, out):
    lanes = lax.broadcasted_iota(jnp.int32, (LM, NY), 1)
    acc = jnp.zeros((LM, NY), jnp.float32)
    for j in range(NY):
        p = pick[b, j]
        row = u3[pl.ds(pl.multiple_of(lax.shift_right_logical(p, 7), LM), LM), :]
        acc = jnp.where(lanes == j, pltpu.roll(row, p & 127, 1), acc)
    out[b] = acc


def put_row(ref, row, value):
    ref[pl.ds(pl.multiple_of(row * LM, LM), LM), :] = value


def clear_edges(ref, e):
    zero = jnp.zeros((LM, NY), jnp.float32)
    put(ref, e, 0, zero)
    put(ref, e, ROWS - 1, zero)


def address(where, place, shift, low, high):
    plane = where >> 14
    row = jnp.where((plane >= low) & (plane <= high), (where >> 7) + shift * NX, 8 * NX)
    return (row << 10) | ((place - where) & 127)


def pack_kernel(lc, cells, upward, downward, near, held, sems):
    copies = [pltpu.make_async_copy(cells, held, sems.at[0])]
    for z in range(3):
        part = pl.ds(NX * z, NX)
        copies.append(pltpu.make_async_copy(lc.at[z + 1], upward.at[part], sems.at[1 + z]))
        copies.append(pltpu.make_async_copy(lc.at[z], downward.at[part], sems.at[4 + z]))
    for copy in copies:
        copy.start()
    copies[0].wait()
    where = held[...]
    upward[3 * NX :] = where.astype(jnp.float32)
    downward[3 * NX :] = where.astype(jnp.float32)
    place = lax.broadcasted_iota(jnp.int32, (8, NY), 1)
    near[...] = address(where, place, 0, 0, 3)
    for copy in copies[1:]:
        copy.wait()


def outer_kernel(far, lc, hs, before, after, modes, share, coef, u1, u2, u3, pick, sem):
    fetch = pltpu.make_async_copy(far, pick, sem)
    fetch.start()
    slab = lax.axis_index("slab_0") * 8 + lax.axis_index("slab_1")
    first = slab == 0
    last = slab == 63
    rows = lax.broadcasted_iota(jnp.int32, (NX, NY), 0)
    cols = lax.broadcasted_iota(jnp.int32, (NX, NY), 1)
    zero = jnp.zeros((LM, NY), jnp.float32)

    own = [jnp.exp(lc[z]) for z in range(CZ)]
    cond = [jnp.where(first, own[0], jnp.exp(before[NX * z : NX * z + NX])) for z in range(3)]
    cond += own
    cond += [jnp.where(last, own[CZ - 1], jnp.exp(after[NX * z : NX * z + NX])) for z in range(3)]
    faces = [harmonic(cond[z], cond[z + 1]) for z in range(9)]

    for e in range(8):
        c = cond[e + 1]
        lower = faces[e]
        upper = faces[e + 1]
        toward_e = jnp.where(rows == NX - 1, c, pltpu.roll(c, NX - 1, 0))
        east = harmonic(c, toward_e)
        west = jnp.where(rows == 0, c, pltpu.roll(east, 1, 0))
        toward_n = jnp.where(cols == NY - 1, c, pltpu.roll(c, NY - 1, 1))
        north = harmonic(c, toward_n)
        south = jnp.where(cols == 0, c, pltpu.roll(north, 1, 1))
        diag = STORAGE + lower + upper + west + east + south + north
        inv = 1.0 / diag
        scale = inv * W2
        if e == 1:
            scale = jnp.where(first, 0.0, scale)
        if e == 6:
            scale = jnp.where(last, 0.0, scale)
        coef[0, e] = lower * scale
        coef[1, e] = upper * scale
        if 1 <= e <= 6:
            coef[2, e] = jnp.where(rows == 0, 0.0, west * scale)
            coef[3, e] = jnp.where(rows == NX - 1, 0.0, east * scale)
            coef[4, e] = jnp.where(cols == 0, 0.0, south * scale)
            coef[5, e] = jnp.where(cols == NY - 1, 0.0, north * scale)
            clear_edges(u2, e)
        if 2 <= e <= 5:
            clear_edges(u1, e)
            lead = hs[e - 2] * c * inv * W1
            for k in range(LM):
                m = modes[k, e - 2].astype(jnp.float32)
                u1[pl.ds((e * ROWS + 1) * LM + k, NX, stride=LM), :] = m * lead

    def clear(i, _):
        for j in range(13):
            x = i * 13 + j
            put(u1, 1, x, zero)
            put(u1, 6, x, zero)
            put(u2, 0, x, zero)
            put(u2, 7, x, zero)
        return 0

    lax.fori_loop(0, ROWS // 13, clear, 0)
    for j in range(8):
        put_row(u3, 8 * NX + j, zero)

    def c(i, e, x):
        return coef[i, e, pl.ds(x - 1, 1), :]

    def end_two(e, x):
        put(u2, 1, x, c(1, 1, x) * at(u1, 2, x))
        put(u2, 6, x, c(0, 6, x) * at(u1, 5, x))

    over_rows((0, 0, 1), 16, end_two)
    over_rows((2, 3, 2), 64, functools.partial(second_row, coef, u1, u2))

    def end_three(e, x):
        put_row(u3, x - 1, (W3 / W2) * (c(1, 0, x) * at(u2, 1, x)))
        put_row(u3, 7 * NX + x - 1, (W3 / W2) * (c(0, 7, x) * at(u2, 6, x)))

    over_rows((0, 0, 1), 16, end_three)

    def third(e, x):
        u, total = sweep(coef, u2, e, x)
        put_row(u3, e * NX + x - 1, (1.0 - W3) * u + (W3 / W2) * total)

    over_rows((1, 5, 2), 64, third)
    fetch.wait()

    def block(b, _):
        pick_block(pick, u3, b, share)
        return 0

    lax.fori_loop(0, 16, block, 0)


def inner_kernel(near, coef, u1, u2, out, w2, u3, pick, sem):
    fetch = pltpu.make_async_copy(near, pick, sem)
    fetch.start()

    def second(e, x):
        u, total = sweep(coef, u1, e, x)
        put(w2, e - 2, x, OWN2 * u + total)

    clear_edges(w2, 1)
    clear_edges(w2, 2)
    over_rows((3, 1, 2), 64, second)

    def third(e, x, here, below, above):
        def c(i):
            return coef[i, e, pl.ds(x - 1, 1), :]

        u = here(x)
        total = c(0) * below(x) + c(1) * above(x)
        total = total + (c(2) * here(x - 1) + c(3) * here(x + 1))
        total = total + (c(4) * pltpu.roll(u, 1, 1) + c(5) * pltpu.roll(u, NY - 1, 1))
        value = (1.0 - W3) * u + (W3 / W1) * at(u1, e, x) + (W3 / W2) * total
        put_row(u3, (e - 2) * NX + x - 1, value)

    def plane(ref, e):
        return lambda x: at(ref, e, x)

    lines = {e: plane(u2, e) for e in (1, 2, 5, 6)}
    lines.update({e: plane(w2, e - 2) for e in (3, 4)})
    for q in range(4):
        over_rows(
            (q + 2, 0, 1),
            64,
            lambda e, x, q=q: third(q + 2, x, lines[q + 2], lines[q + 1], lines[q + 3]),
        )

    fetch.wait()

    def block(b, _):
        pick_block(pick, u3, b, out)
        return 0

    lax.fori_loop(0, 8, block, 0)


def gram_kernel(resp, var, misfit, out):
    r = resp[...]
    scaled = r / var[...]
    mis = misfit[...]
    half = MODES // 2
    none = jnp.zeros((half, OBS), jnp.float32)
    none_f = jnp.zeros((FIELDS, OBS), jnp.float32)
    right_a = jnp.concatenate([r, none, mis, none_f], axis=0)
    right_b = jnp.concatenate([none, none, r[half:], none_f, mis], axis=0)
    dims = (((1,), (1,)), ((), ()))
    got = lax.dot_general(scaled[:half], right_a, dims, precision=HI, preferred_element_type=jnp.float32)
    got = got + lax.dot_general(
        scaled[half:], right_b, dims, precision=HI, preferred_element_type=jnp.float32
    )
    for d in range(8):
        out[d] = got


def total_kernel(parts, out):
    got = parts[0]
    for d in range(1, 8):
        got = got + parts[d]
    for d in range(8):
        out[d] = got


def solve_kernel(parts, out):
    p = parts[0]
    for d in range(1, 8):
        p = p + parts[d]
    half = MODES // 2
    lane = lax.broadcasted_iota(jnp.int32, (half, 128), 1)
    square = jnp.concatenate([p, jnp.zeros((128 - half, 128), jnp.float32)], axis=0)
    turned = square.T[half : 2 * half]
    near = pltpu.roll(p, 128 - 32, 1)
    far = pltpu.roll(p, 128 - 48, 1)
    top = jnp.where(lane < 64, p, near)
    low = jnp.where(lane < 32, turned, jnp.where(lane < 64, near, far))
    a = jnp.concatenate([top, low], axis=0)
    row = lax.broadcasted_iota(jnp.int32, (MODES, 128), 0)
    col = lax.broadcasted_iota(jnp.int32, (MODES, 128), 1)
    a = jnp.where(row == col, a + 1.0, a)
    a = [a[8 * i : 8 * i + 8] for i in range(8)]
    sub = lax.broadcasted_iota(jnp.int32, (8, 128), 0)

    def wide(v):
        return jnp.broadcast_to(v, (8, 128))

    for q in range(8):
        cs = [[wide(a[i][:, 8 * q + t : 8 * q + t + 1]) for i in range(8)] for t in range(8)]
        for t in range(8):
            c = cs[t]
            inv = 1.0 / wide(c[q][t : t + 1])
            norm = wide(a[q][t : t + 1]) * inv
            for i in range(8):
                new = a[i] - c[i] * norm
                a[i] = jnp.where(sub == t, norm, new) if i == q else new
            for s in range(t + 1, 8):
                f = wide(c[q][s : s + 1]) * inv
                for i in range(8):
                    new = cs[s][i] - c[i] * f
                    cs[s][i] = jnp.where(sub == t, f, new) if i == q else new
    for i in range(8):
        out[8 * i : 8 * i + 8, :] = a[i]


def vmem(n):
    return [pl.BlockSpec(memory_space=pltpu.VMEM)] * n


def smem(n):
    return [pl.BlockSpec(memory_space=pltpu.SMEM)] * n


def stay(x):
    return pltpu.with_memory_space_constraint(x, pltpu.HBM)


def limit(mib):
    return pltpu.CompilerParams(vmem_limit_bytes=mib * 1024 * 1024)


def on_device(log_cond, head_slope, modes, obs_cells, obs_var, misfit, base_fields):
    slabs = lax.axis_size(SLAB)
    ahead = [(i, i + 1) for i in range(slabs - 1)]
    back = [(i + 1, i) for i in range(slabs - 1)]

    message = jax.ShapeDtypeStruct((3 * NX + 8, NY), jnp.float32)
    upward, downward, near_pick = pl.pallas_call(
        pack_kernel,
        out_shape=(message, message, jax.ShapeDtypeStruct((8, NY), jnp.int32)),
        in_specs=[pl.BlockSpec(memory_space=pltpu.HBM)] * 2,
        out_specs=vmem(3),
        scratch_shapes=[pltpu.VMEM((8, NY), jnp.int32), pltpu.SemaphoreType.DMA((7,))],
        compiler_params=limit(4),
        name="pack",
    )(stay(log_cond), stay(obs_cells.reshape(8, NY)))
    before = lax.ppermute(upward, SLAB, ahead)
    after = lax.ppermute(downward, SLAB, back)

    pieces = jnp.moveaxis(modes.reshape(LM, CZ, 8, NX // 8, NY), 2, 0)
    block = lax.all_to_all(pieces, MODE, 0, 0, tiled=True)

    place = lax.broadcasted_iota(jnp.int32, (8, NY), 1)

    def arrived(x):
        return x[3 * NX :].astype(jnp.int32)

    far_pick = jnp.concatenate(
        [address(arrived(before), place, -2, 2, 3), address(arrived(after), place, 6, 0, 1)]
    )
    plane_rows = jax.ShapeDtypeStruct((8 * ROWS * LM, NY), jnp.float32)
    share, coefs, u1, u2 = pl.pallas_call(
        outer_kernel,
        out_shape=(
            jax.ShapeDtypeStruct((16, LM, NY), jnp.float32),
            jax.ShapeDtypeStruct((6, 8, NX, NY), jnp.float32),
            plane_rows,
            plane_rows,
        ),
        in_specs=vmem(6),
        out_specs=vmem(4),
        scratch_shapes=[
            pltpu.VMEM(((8 * NX + 8) * LM, NY), jnp.float32),
            pltpu.SMEM((16, NY), jnp.int32),
            pltpu.SemaphoreType.DMA,
        ],
        compiler_params=limit(24),
        name="outer",
    )(far_pick, log_cond, head_slope, before, after, modes)
    from_above = lax.ppermute(share[:8], SLAB, back)
    from_below = lax.ppermute(share[8:], SLAB, ahead)
    picked = pl.pallas_call(
        inner_kernel,
        out_shape=jax.ShapeDtypeStruct((8, LM, NY), jnp.float32),
        in_specs=vmem(4),
        out_specs=vmem(1)[0],
        scratch_shapes=[
            pltpu.VMEM((4 * ROWS * LM, NY), jnp.float32),
            pltpu.VMEM((4 * NX * LM, NY), jnp.float32),
            pltpu.SMEM((8, NY), jnp.int32),
            pltpu.SemaphoreType.DMA,
        ],
        compiler_params=limit(24),
        name="inner",
    )(near_pick, coefs, u1, u2)
    block, from_above, from_below = lax.optimization_barrier((block, from_above, from_below))
    picked = picked + from_above + from_below
    copies = jnp.broadcast_to(picked, (8, 8, LM, NY))
    whole = lax.all_to_all(copies, MODE, 0, 0, tiled=True)
    whole = jnp.moveaxis(whole, 1, 2).reshape(MODES, OBS)

    shared = jax.ShapeDtypeStruct((8, 32, 128), jnp.float32)
    part = pl.pallas_call(gram_kernel, out_shape=shared, in_specs=vmem(3), out_specs=vmem(1)[0], compiler_params=limit(6), name="gram")(
        whole, obs_var.reshape(1, OBS), misfit.T
    )
    part = lax.all_to_all(part, "slab_1", 0, 0, tiled=True)
    part = pl.pallas_call(total_kernel, out_shape=shared, in_specs=vmem(1), out_specs=vmem(1)[0], compiler_params=limit(4), name="total")(part)
    part = lax.all_to_all(part, "slab_0", 0, 0, tiled=True)
    solved = pl.pallas_call(
        solve_kernel,
        out_shape=jax.ShapeDtypeStruct((MODES, 128), jnp.float32),
        in_specs=vmem(1),
        out_specs=vmem(1)[0],
        compiler_params=limit(4),
        name="solve",
    )(part)
    coef = solved[:, MODES : MODES + FIELDS]

    layer = block.reshape(MODES, CZ, NX // 8, NY).astype(jnp.float32)
    update = lax.dot_general(coef, layer, (((0,), (0,)), ((), ())), precision=HI)
    return base_fields.astype(jnp.float32) + update


def solution(mesh):
    torus = Mesh(mesh.devices.reshape(4, 2, 8, 8), ("mode_0", "mode_1", "slab_0", "slab_1"))
    in_specs = (
        P(SLAB, None, None),
        P(SLAB, None, None),
        P(MODE, SLAB, None, None),
        P(SLAB),
        P(SLAB),
        P(SLAB, None),
        P(None, SLAB, MODE, None),
    )
    out_specs = P(None, SLAB, MODE, None)
    return jax.shard_map(
        on_device, mesh=torus, in_specs=in_specs, out_specs=out_specs, check_vma=False
    )
```

```python
import functools
import math

import jax
import jax.numpy as jnp
from jax import lax
from jax.experimental import pallas as pl
from jax.experimental.pallas import tpu as pltpu
from jax.sharding import Mesh
from jax.sharding import PartitionSpec as P


ITERS = 3
SLAB = ("slab_0", "slab_1")
MODE = ("mode_0", "mode_1")
STORAGE = 0.05
CZ = 4
NX = 128
NY = 128
LM = 8
OBS = 1024
MODES = 64
FIELDS = 16
ROWS = NX + 2
HI = lax.Precision.HIGHEST


def sweep_weights(count):
    order = []
    low, high = (0, count - 1)
    while low <= high:
        order.append(low)
        if high != low:
            order.append(high)
        low += 1
        high -= 1
    return [1.0 / (1.15 + 0.85 * math.cos((2 * i + 1) * math.pi / (2 * count))) for i in order]


W1, W2, W3 = sweep_weights(ITERS)
OWN2 = 1.0 - W2 + W2 / W1


def harmonic(a, b):
    return 2.0 * a * b / (a + b)


def at(ref, e, x):
    return ref[pl.ds(pl.multiple_of((e * ROWS + x) * LM, LM), LM), :]


def put(ref, e, x, value):
    ref[pl.ds(pl.multiple_of((e * ROWS + x) * LM, LM), LM), :] = value


def sweep(coef, ref, e, x):
    def c(i):
        return coef[i, e, pl.ds(x - 1, 1), :]

    u = at(ref, e, x)
    total = c(0) * at(ref, e - 1, x) + c(1) * at(ref, e + 1, x)
    total = total + (c(2) * at(ref, e, x - 1) + c(3) * at(ref, e, x + 1))
    total = total + (c(4) * pltpu.roll(u, 1, 1) + c(5) * pltpu.roll(u, NY - 1, 1))
    return u, total


def over_rows(planes, unroll, fn):
    first, step, count = planes
    pieces = NX // unroll

    def body(i, _):
        e = first + step * (i // pieces)
        start = (i % pieces) * unroll + 1
        for j in range(unroll):
            fn(e, start + j)
        return 0

    lax.fori_loop(0, count * pieces, body, 0)


def second_row(coef, u1, u2, e, x):
    u, total = sweep(coef, u1, e, x)
    put(u2, e, x, OWN2 * u + total)


def pick_block(buf, u3, b, out):
    lanes = lax.broadcasted_iota(jnp.int32, (LM, NY), 1)
    acc = jnp.zeros((LM, NY), jnp.float32)
    for j in range(NY):
        p = buf[0, j]
        row = u3[pl.ds(pl.multiple_of(lax.shift_right_logical(p, 7), LM), LM), :]
        acc = jnp.where(lanes == j, pltpu.roll(row, p & 127, 1), acc)
    out[b] = acc


def fetches(picks, bufs, sems):
    return [pltpu.make_async_copy(picks.at[q], buf, sems.at[q]) for q, buf in enumerate(bufs)]


def pick_all(picks, bufs, sems, u3, out):
    for fetch in fetches(picks, bufs, sems):
        fetch.wait()
    for q, buf in enumerate(bufs):
        pick_block(buf, u3, q, out)


def put_row(ref, row, value):
    ref[pl.ds(pl.multiple_of(row * LM, LM), LM), :] = value


def clear_edges(ref, e):
    zero = jnp.zeros((LM, NY), jnp.float32)
    put(ref, e, 0, zero)
    put(ref, e, ROWS - 1, zero)


def address(where, place, shift, low, high):
    plane = where >> 14
    row = jnp.where((plane >= low) & (plane <= high), (where >> 7) + shift * NX, 8 * NX)
    return (row << 10) | ((place - where) & 127)


def pack_kernel(lc, cells, upward, downward, near, held, sems):
    copies = [pltpu.make_async_copy(cells, held, sems.at[0])]
    for z in range(3):
        part = pl.ds(NX * z, NX)
        copies.append(pltpu.make_async_copy(lc.at[z + 1], upward.at[part], sems.at[1 + z]))
        copies.append(pltpu.make_async_copy(lc.at[z], downward.at[part], sems.at[4 + z]))
    for copy in copies:
        copy.start()
    copies[0].wait()
    where = held[...]
    upward[3 * NX :] = where.astype(jnp.float32)
    downward[3 * NX :] = where.astype(jnp.float32)
    place = lax.broadcasted_iota(jnp.int32, (8, NY), 1)
    spot = address(where, place, 0, 0, 3)
    for q in range(8):
        near[q] = spot[q : q + 1]
    for copy in copies[1:]:
        copy.wait()


def outer_kernel(far, lc, hs, before, after, modes, share, coef, u1, u2, u3, sems, *bufs):
    for fetch in fetches(far, bufs, sems):
        fetch.start()
    slab = lax.axis_index("slab_0") * 8 + lax.axis_index("slab_1")
    first = slab == 0
    last = slab == 63
    rows = lax.broadcasted_iota(jnp.int32, (NX, NY), 0)
    cols = lax.broadcasted_iota(jnp.int32, (NX, NY), 1)
    zero = jnp.zeros((LM, NY), jnp.float32)

    own = [jnp.exp(lc[z]) for z in range(CZ)]
    cond = [jnp.where(first, own[0], jnp.exp(before[NX * z : NX * z + NX])) for z in range(3)]
    cond += own
    cond += [jnp.where(last, own[CZ - 1], jnp.exp(after[NX * z : NX * z + NX])) for z in range(3)]
    faces = [harmonic(cond[z], cond[z + 1]) for z in range(9)]

    for e in range(8):
        c = cond[e + 1]
        lower = faces[e]
        upper = faces[e + 1]
        toward_e = jnp.where(rows == NX - 1, c, pltpu.roll(c, NX - 1, 0))
        east = harmonic(c, toward_e)
        west = jnp.where(rows == 0, c, pltpu.roll(east, 1, 0))
        toward_n = jnp.where(cols == NY - 1, c, pltpu.roll(c, NY - 1, 1))
        north = harmonic(c, toward_n)
        south = jnp.where(cols == 0, c, pltpu.roll(north, 1, 1))
        diag = STORAGE + lower + upper + west + east + south + north
        inv = 1.0 / diag
        scale = inv * W2
        if e == 1:
            scale = jnp.where(first, 0.0, scale)
        if e == 6:
            scale = jnp.where(last, 0.0, scale)
        coef[0, e] = lower * scale
        coef[1, e] = upper * scale
        if 1 <= e <= 6:
            coef[2, e] = jnp.where(rows == 0, 0.0, west * scale)
            coef[3, e] = jnp.where(rows == NX - 1, 0.0, east * scale)
            coef[4, e] = jnp.where(cols == 0, 0.0, south * scale)
            coef[5, e] = jnp.where(cols == NY - 1, 0.0, north * scale)
            clear_edges(u2, e)
        if 2 <= e <= 5:
            clear_edges(u1, e)
            lead = hs[e - 2] * c * inv * W1
            for k in range(LM):
                m = modes[k, e - 2].astype(jnp.float32)
                u1[pl.ds((e * ROWS + 1) * LM + k, NX, stride=LM), :] = m * lead

    def clear(i, _):
        for j in range(13):
            x = i * 13 + j
            put(u1, 1, x, zero)
            put(u1, 6, x, zero)
            put(u2, 0, x, zero)
            put(u2, 7, x, zero)
        return 0

    lax.fori_loop(0, ROWS // 13, clear, 0)
    for j in range(8):
        put_row(u3, 8 * NX + j, zero)

    def c(i, e, x):
        return coef[i, e, pl.ds(x - 1, 1), :]

    def end_two(e, x):
        put(u2, 1, x, c(1, 1, x) * at(u1, 2, x))
        put(u2, 6, x, c(0, 6, x) * at(u1, 5, x))

    over_rows((0, 0, 1), 16, end_two)
    over_rows((2, 3, 2), 64, functools.partial(second_row, coef, u1, u2))

    def end_three(e, x):
        put_row(u3, x - 1, (W3 / W2) * (c(1, 0, x) * at(u2, 1, x)))
        put_row(u3, 7 * NX + x - 1, (W3 / W2) * (c(0, 7, x) * at(u2, 6, x)))

    over_rows((0, 0, 1), 16, end_three)

    def third(e, x):
        u, total = sweep(coef, u2, e, x)
        put_row(u3, e * NX + x - 1, (1.0 - W3) * u + (W3 / W2) * total)

    over_rows((1, 5, 2), 64, third)
    pick_all(far, bufs, sems, u3, share)


def inner_kernel(near, coef, u1, u2, out, w2, u3, sems, *bufs):
    for fetch in fetches(near, bufs, sems):
        fetch.start()

    def second(e, x):
        u, total = sweep(coef, u1, e, x)
        put(w2, e - 2, x, OWN2 * u + total)

    clear_edges(w2, 1)
    clear_edges(w2, 2)
    over_rows((3, 1, 2), 64, second)

    def third(e, x, here, below, above):
        def c(i):
            return coef[i, e, pl.ds(x - 1, 1), :]

        u = here(x)
        total = c(0) * below(x) + c(1) * above(x)
        total = total + (c(2) * here(x - 1) + c(3) * here(x + 1))
        total = total + (c(4) * pltpu.roll(u, 1, 1) + c(5) * pltpu.roll(u, NY - 1, 1))
        value = (1.0 - W3) * u + (W3 / W1) * at(u1, e, x) + (W3 / W2) * total
        put_row(u3, (e - 2) * NX + x - 1, value)

    def plane(ref, e):
        return lambda x: at(ref, e, x)

    lines = {e: plane(u2, e) for e in (1, 2, 5, 6)}
    lines.update({e: plane(w2, e - 2) for e in (3, 4)})
    for q in range(4):
        over_rows(
            (q + 2, 0, 1),
            64,
            lambda e, x, q=q: third(q + 2, x, lines[q + 2], lines[q + 1], lines[q + 3]),
        )

    pick_all(near, bufs, sems, u3, out)


def gram_kernel(resp, var, misfit, out):
    r = resp[...]
    scaled = r / var[...]
    mis = misfit[...]
    half = MODES // 2
    none = jnp.zeros((half, OBS), jnp.float32)
    none_f = jnp.zeros((FIELDS, OBS), jnp.float32)
    right_a = jnp.concatenate([r, none, mis, none_f], axis=0)
    right_b = jnp.concatenate([none, none, r[half:], none_f, mis], axis=0)
    dims = (((1,), (1,)), ((), ()))
    got = lax.dot_general(scaled[:half], right_a, dims, precision=HI, preferred_element_type=jnp.float32)
    got = got + lax.dot_general(
        scaled[half:], right_b, dims, precision=HI, preferred_element_type=jnp.float32
    )
    for d in range(8):
        out[d] = got


def total_kernel(parts, out):
    got = parts[0]
    for d in range(1, 8):
        got = got + parts[d]
    for d in range(8):
        out[d] = got


def solve_kernel(parts, out):
    p = parts[0]
    for d in range(1, 8):
        p = p + parts[d]
    half = MODES // 2
    lane = lax.broadcasted_iota(jnp.int32, (half, 128), 1)
    square = jnp.concatenate([p, jnp.zeros((128 - half, 128), jnp.float32)], axis=0)
    turned = square.T[half : 2 * half]
    near = pltpu.roll(p, 128 - 32, 1)
    far = pltpu.roll(p, 128 - 48, 1)
    top = jnp.where(lane < 64, p, near)
    low = jnp.where(lane < 32, turned, jnp.where(lane < 64, near, far))
    a = jnp.concatenate([top, low], axis=0)
    row = lax.broadcasted_iota(jnp.int32, (MODES, 128), 0)
    col = lax.broadcasted_iota(jnp.int32, (MODES, 128), 1)
    a = jnp.where(row == col, a + 1.0, a)
    a = [a[8 * i : 8 * i + 8] for i in range(8)]
    sub = lax.broadcasted_iota(jnp.int32, (8, 128), 0)

    def wide(v):
        return jnp.broadcast_to(v, (8, 128))

    for q in range(8):
        cs = [[wide(a[i][:, 8 * q + t : 8 * q + t + 1]) for i in range(8)] for t in range(8)]
        for t in range(8):
            c = cs[t]
            inv = 1.0 / wide(c[q][t : t + 1])
            norm = wide(a[q][t : t + 1]) * inv
            for i in range(8):
                new = a[i] - c[i] * norm
                a[i] = jnp.where(sub == t, norm, new) if i == q else new
            for s in range(t + 1, 8):
                f = wide(c[q][s : s + 1]) * inv
                for i in range(8):
                    new = cs[s][i] - c[i] * f
                    cs[s][i] = jnp.where(sub == t, f, new) if i == q else new
    for i in range(8):
        out[8 * i : 8 * i + 8, :] = a[i]


def vmem(n):
    return [pl.BlockSpec(memory_space=pltpu.VMEM)] * n


def stay(x):
    return pltpu.with_memory_space_constraint(x, pltpu.HBM)


def limit(mib):
    return pltpu.CompilerParams(vmem_limit_bytes=mib * 1024 * 1024)


def on_device(log_cond, head_slope, modes, obs_cells, obs_var, misfit, base_fields):
    slabs = lax.axis_size(SLAB)
    ahead = [(i, i + 1) for i in range(slabs - 1)]
    back = [(i + 1, i) for i in range(slabs - 1)]

    message = jax.ShapeDtypeStruct((3 * NX + 8, NY), jnp.float32)
    upward, downward, near_pick = pl.pallas_call(
        pack_kernel,
        out_shape=(message, message, jax.ShapeDtypeStruct((8, 1, NY), jnp.int32)),
        in_specs=[pl.BlockSpec(memory_space=pltpu.HBM)] * 2,
        out_specs=vmem(3),
        scratch_shapes=[pltpu.VMEM((8, NY), jnp.int32), pltpu.SemaphoreType.DMA((7,))],
        compiler_params=limit(4),
        name="pack",
    )(stay(log_cond), stay(obs_cells.reshape(8, NY)))
    before = lax.ppermute(upward, SLAB, ahead)
    after = lax.ppermute(downward, SLAB, back)

    pieces = jnp.moveaxis(modes.reshape(LM, CZ, 8, NX // 8, NY), 2, 0)
    block = lax.all_to_all(pieces, MODE, 0, 0, tiled=True)

    place = lax.broadcasted_iota(jnp.int32, (8, NY), 1)

    def arrived(x):
        return x[3 * NX :].astype(jnp.int32)

    far_pick = jnp.concatenate(
        [address(arrived(before), place, -2, 2, 3), address(arrived(after), place, 6, 0, 1)]
    ).reshape(16, 1, NY)
    plane_rows = jax.ShapeDtypeStruct((8 * ROWS * LM, NY), jnp.float32)
    share, coefs, u1, u2 = pl.pallas_call(
        outer_kernel,
        out_shape=(
            jax.ShapeDtypeStruct((16, LM, NY), jnp.float32),
            jax.ShapeDtypeStruct((6, 8, NX, NY), jnp.float32),
            plane_rows,
            plane_rows,
        ),
        in_specs=vmem(6),
        out_specs=vmem(4),
        scratch_shapes=[
            pltpu.VMEM(((8 * NX + 8) * LM, NY), jnp.float32),
            pltpu.SemaphoreType.DMA((16,)),
            *[pltpu.SMEM((1, NY), jnp.int32)] * 16,
        ],
        compiler_params=limit(24),
        name="outer",
    )(far_pick, log_cond, head_slope, before, after, modes)
    from_above = lax.ppermute(share[:8], SLAB, back)
    from_below = lax.ppermute(share[8:], SLAB, ahead)
    picked = pl.pallas_call(
        inner_kernel,
        out_shape=jax.ShapeDtypeStruct((8, LM, NY), jnp.float32),
        in_specs=vmem(4),
        out_specs=vmem(1)[0],
        scratch_shapes=[
            pltpu.VMEM((4 * ROWS * LM, NY), jnp.float32),
            pltpu.VMEM((4 * NX * LM, NY), jnp.float32),
            pltpu.SemaphoreType.DMA((8,)),
            *[pltpu.SMEM((1, NY), jnp.int32)] * 8,
        ],
        compiler_params=limit(24),
        name="inner",
    )(near_pick, coefs, u1, u2)
    block, from_above, from_below = lax.optimization_barrier((block, from_above, from_below))
    picked = picked + from_above + from_below
    copies = jnp.broadcast_to(picked, (8, 8, LM, NY))
    whole = lax.all_to_all(copies, MODE, 0, 0, tiled=True)
    whole = jnp.moveaxis(whole, 1, 2).reshape(MODES, OBS)

    shared = jax.ShapeDtypeStruct((8, 32, 128), jnp.float32)
    part = pl.pallas_call(gram_kernel, out_shape=shared, in_specs=vmem(3), out_specs=vmem(1)[0], compiler_params=limit(6), name="gram")(
        whole, obs_var.reshape(1, OBS), misfit.T
    )
    part = lax.all_to_all(part, "slab_1", 0, 0, tiled=True)
    part = pl.pallas_call(total_kernel, out_shape=shared, in_specs=vmem(1), out_specs=vmem(1)[0], compiler_params=limit(4), name="total")(part)
    part = lax.all_to_all(part, "slab_0", 0, 0, tiled=True)
    solved = pl.pallas_call(
        solve_kernel,
        out_shape=jax.ShapeDtypeStruct((MODES, 128), jnp.float32),
        in_specs=vmem(1),
        out_specs=vmem(1)[0],
        compiler_params=limit(4),
        name="solve",
    )(part)
    coef = solved[:, MODES : MODES + FIELDS]

    layer = block.reshape(MODES, CZ, NX // 8, NY).astype(jnp.float32)
    update = lax.dot_general(coef, layer, (((0,), (0,)), ((), ())), precision=HI)
    return base_fields.astype(jnp.float32) + update


def solution(mesh):
    torus = Mesh(mesh.devices.reshape(4, 2, 8, 8), ("mode_0", "mode_1", "slab_0", "slab_1"))
    in_specs = (
        P(SLAB, None, None),
        P(SLAB, None, None),
        P(MODE, SLAB, None, None),
        P(SLAB),
        P(SLAB),
        P(SLAB, None),
        P(None, SLAB, MODE, None),
    )
    out_specs = P(None, SLAB, MODE, None)
    return jax.shard_map(
        on_device, mesh=torus, in_specs=in_specs, out_specs=out_specs, check_vma=False
    )
```

```python
import functools
import math

import jax
import jax.numpy as jnp
from jax import lax
from jax.experimental import pallas as pl
from jax.experimental.pallas import tpu as pltpu
from jax.sharding import Mesh
from jax.sharding import PartitionSpec as P


ITERS = 3
SLAB = ("slab_0", "slab_1")
MODE = ("mode_0", "mode_1")
STORAGE = 0.05
CZ = 4
NX = 128
NY = 128
LM = 8
OBS = 1024
MODES = 64
FIELDS = 16
ROWS = NX + 2
HI = lax.Precision.HIGHEST


def sweep_weights(count):
    order = []
    low, high = (0, count - 1)
    while low <= high:
        order.append(low)
        if high != low:
            order.append(high)
        low += 1
        high -= 1
    return [1.0 / (1.15 + 0.85 * math.cos((2 * i + 1) * math.pi / (2 * count))) for i in order]


W1, W2, W3 = sweep_weights(ITERS)
OWN2 = 1.0 - W2 + W2 / W1


def harmonic(a, b):
    return 2.0 * a * b / (a + b)


def at(ref, e, x):
    return ref[pl.ds(pl.multiple_of((e * ROWS + x) * LM, LM), LM), :]


def put(ref, e, x, value):
    ref[pl.ds(pl.multiple_of((e * ROWS + x) * LM, LM), LM), :] = value


def sweep(coef, ref, e, x):
    def c(i):
        return coef[i, e, pl.ds(x - 1, 1), :]

    u = at(ref, e, x)
    total = c(0) * at(ref, e - 1, x) + c(1) * at(ref, e + 1, x)
    total = total + (c(2) * at(ref, e, x - 1) + c(3) * at(ref, e, x + 1))
    total = total + (c(4) * pltpu.roll(u, 1, 1) + c(5) * pltpu.roll(u, NY - 1, 1))
    return u, total


def over_rows(planes, unroll, fn):
    first, step, count = planes
    pieces = NX // unroll

    def body(i, _):
        e = first + step * (i // pieces)
        start = (i % pieces) * unroll + 1
        for j in range(unroll):
            fn(e, start + j)
        return 0

    lax.fori_loop(0, count * pieces, body, 0)


def second_row(coef, u1, u2, e, x):
    u, total = sweep(coef, u1, e, x)
    put(u2, e, x, OWN2 * u + total)


def pick_block(buf, u3, b, out):
    lanes = lax.broadcasted_iota(jnp.int32, (LM, NY), 1)
    acc = jnp.zeros((LM, NY), jnp.float32)
    for j in range(NY):
        p = buf[0, j]
        row = u3[pl.ds(pl.multiple_of(lax.shift_right_logical(p, 7), LM), LM), :]
        acc = jnp.where(lanes == j, pltpu.roll(row, p & 127, 1), acc)
    out[b] = acc


def fetches(picks, bufs, sems):
    return [pltpu.make_async_copy(picks.at[q], buf, sems.at[q]) for q, buf in enumerate(bufs)]


def pick_all(picks, bufs, sems, u3, out):
    for fetch in fetches(picks, bufs, sems):
        fetch.wait()
    for q, buf in enumerate(bufs):
        pick_block(buf, u3, q, out)


def put_row(ref, row, value):
    ref[pl.ds(pl.multiple_of(row * LM, LM), LM), :] = value


def clear_edges(ref, e):
    zero = jnp.zeros((LM, NY), jnp.float32)
    put(ref, e, 0, zero)
    put(ref, e, ROWS - 1, zero)


def address(where, place, shift, low, high):
    plane = where >> 14
    row = jnp.where((plane >= low) & (plane <= high), (where >> 7) + shift * NX, 8 * NX)
    return (row << 10) | ((place - where) & 127)


def pack_kernel(lc, cells, modes, upward, downward, near, modes_near, held, sems):
    copies = [pltpu.make_async_copy(cells, held, sems.at[0])]
    for z in range(3):
        part = pl.ds(NX * z, NX)
        copies.append(pltpu.make_async_copy(lc.at[z + 1], upward.at[part], sems.at[1 + z]))
        copies.append(pltpu.make_async_copy(lc.at[z], downward.at[part], sems.at[4 + z]))
    for k in range(LM):
        copies.append(pltpu.make_async_copy(modes.at[k], modes_near.at[k], sems.at[7 + k]))
    for copy in copies:
        copy.start()
    copies[0].wait()
    where = held[...]
    upward[3 * NX :] = where.astype(jnp.float32)
    downward[3 * NX :] = where.astype(jnp.float32)
    place = lax.broadcasted_iota(jnp.int32, (8, NY), 1)
    spot = address(where, place, 0, 0, 3)
    for q in range(8):
        near[q] = spot[q : q + 1]
    for copy in copies[1:]:
        copy.wait()


def pieces_kernel(modes, out, held, sems):
    copies = [pltpu.make_async_copy(held.at[d], out.at[d], sems.at[d]) for d in range(8)]
    for d in range(8):
        held[d] = modes[:, :, 16 * d : 16 * d + 16, :]
        copies[d].start()
    for copy in copies:
        copy.wait()


def outer_kernel(far, lc, hs, before, after, modes, share, coef, u1, u2, u3, sems, *bufs):
    for fetch in fetches(far, bufs, sems):
        fetch.start()
    slab = lax.axis_index("slab_0") * 8 + lax.axis_index("slab_1")
    first = slab == 0
    last = slab == 63
    rows = lax.broadcasted_iota(jnp.int32, (NX, NY), 0)
    cols = lax.broadcasted_iota(jnp.int32, (NX, NY), 1)
    zero = jnp.zeros((LM, NY), jnp.float32)

    own = [jnp.exp(lc[z]) for z in range(CZ)]
    cond = [jnp.where(first, own[0], jnp.exp(before[NX * z : NX * z + NX])) for z in range(3)]
    cond += own
    cond += [jnp.where(last, own[CZ - 1], jnp.exp(after[NX * z : NX * z + NX])) for z in range(3)]
    faces = [harmonic(cond[z], cond[z + 1]) for z in range(9)]

    for e in range(8):
        c = cond[e + 1]
        lower = faces[e]
        upper = faces[e + 1]
        toward_e = jnp.where(rows == NX - 1, c, pltpu.roll(c, NX - 1, 0))
        east = harmonic(c, toward_e)
        west = jnp.where(rows == 0, c, pltpu.roll(east, 1, 0))
        toward_n = jnp.where(cols == NY - 1, c, pltpu.roll(c, NY - 1, 1))
        north = harmonic(c, toward_n)
        south = jnp.where(cols == 0, c, pltpu.roll(north, 1, 1))
        diag = STORAGE + lower + upper + west + east + south + north
        inv = 1.0 / diag
        scale = inv * W2
        if e == 1:
            scale = jnp.where(first, 0.0, scale)
        if e == 6:
            scale = jnp.where(last, 0.0, scale)
        coef[0, e] = lower * scale
        coef[1, e] = upper * scale
        if 1 <= e <= 6:
            coef[2, e] = jnp.where(rows == 0, 0.0, west * scale)
            coef[3, e] = jnp.where(rows == NX - 1, 0.0, east * scale)
            coef[4, e] = jnp.where(cols == 0, 0.0, south * scale)
            coef[5, e] = jnp.where(cols == NY - 1, 0.0, north * scale)
            clear_edges(u2, e)
        if 2 <= e <= 5:
            clear_edges(u1, e)
            lead = hs[e - 2] * c * inv * W1
            for k in range(LM):
                m = modes[k, e - 2].astype(jnp.float32)
                u1[pl.ds((e * ROWS + 1) * LM + k, NX, stride=LM), :] = m * lead

    def clear(i, _):
        for j in range(13):
            x = i * 13 + j
            put(u1, 1, x, zero)
            put(u1, 6, x, zero)
            put(u2, 0, x, zero)
            put(u2, 7, x, zero)
        return 0

    lax.fori_loop(0, ROWS // 13, clear, 0)
    for j in range(8):
        put_row(u3, 8 * NX + j, zero)

    def c(i, e, x):
        return coef[i, e, pl.ds(x - 1, 1), :]

    def end_two(e, x):
        put(u2, 1, x, c(1, 1, x) * at(u1, 2, x))
        put(u2, 6, x, c(0, 6, x) * at(u1, 5, x))

    over_rows((0, 0, 1), 16, end_two)
    over_rows((2, 3, 2), 64, functools.partial(second_row, coef, u1, u2))

    def end_three(e, x):
        put_row(u3, x - 1, (W3 / W2) * (c(1, 0, x) * at(u2, 1, x)))
        put_row(u3, 7 * NX + x - 1, (W3 / W2) * (c(0, 7, x) * at(u2, 6, x)))

    over_rows((0, 0, 1), 16, end_three)

    def third(e, x):
        u, total = sweep(coef, u2, e, x)
        put_row(u3, e * NX + x - 1, (1.0 - W3) * u + (W3 / W2) * total)

    over_rows((1, 5, 2), 64, third)
    pick_all(far, bufs, sems, u3, share)


def inner_kernel(near, coef, u1, u2, out, w2, u3, sems, *bufs):
    for fetch in fetches(near, bufs, sems):
        fetch.start()

    def second(e, x):
        u, total = sweep(coef, u1, e, x)
        put(w2, e - 2, x, OWN2 * u + total)

    clear_edges(w2, 1)
    clear_edges(w2, 2)
    over_rows((3, 1, 2), 64, second)

    def third(e, x, here, below, above):
        def c(i):
            return coef[i, e, pl.ds(x - 1, 1), :]

        u = here(x)
        total = c(0) * below(x) + c(1) * above(x)
        total = total + (c(2) * here(x - 1) + c(3) * here(x + 1))
        total = total + (c(4) * pltpu.roll(u, 1, 1) + c(5) * pltpu.roll(u, NY - 1, 1))
        value = (1.0 - W3) * u + (W3 / W1) * at(u1, e, x) + (W3 / W2) * total
        put_row(u3, (e - 2) * NX + x - 1, value)

    def plane(ref, e):
        return lambda x: at(ref, e, x)

    lines = {e: plane(u2, e) for e in (1, 2, 5, 6)}
    lines.update({e: plane(w2, e - 2) for e in (3, 4)})
    for q in range(4):
        over_rows(
            (q + 2, 0, 1),
            64,
            lambda e, x, q=q: third(q + 2, x, lines[q + 2], lines[q + 1], lines[q + 3]),
        )

    pick_all(near, bufs, sems, u3, out)


def gram_kernel(resp, var, misfit, out):
    r = resp[...]
    scaled = r / var[...]
    mis = misfit[...]
    half = MODES // 2
    none = jnp.zeros((half, OBS), jnp.float32)
    none_f = jnp.zeros((FIELDS, OBS), jnp.float32)
    right_a = jnp.concatenate([r, none, mis, none_f], axis=0)
    right_b = jnp.concatenate([none, none, r[half:], none_f, mis], axis=0)
    dims = (((1,), (1,)), ((), ()))
    got = lax.dot_general(scaled[:half], right_a, dims, precision=HI, preferred_element_type=jnp.float32)
    got = got + lax.dot_general(
        scaled[half:], right_b, dims, precision=HI, preferred_element_type=jnp.float32
    )
    for d in range(8):
        out[d] = got


def total_kernel(parts, out):
    got = parts[0]
    for d in range(1, 8):
        got = got + parts[d]
    for d in range(8):
        out[d] = got


def solve_kernel(parts, out):
    p = parts[0]
    for d in range(1, 8):
        p = p + parts[d]
    half = MODES // 2
    lane = lax.broadcasted_iota(jnp.int32, (half, 128), 1)
    square = jnp.concatenate([p, jnp.zeros((128 - half, 128), jnp.float32)], axis=0)
    turned = square.T[half : 2 * half]
    near = pltpu.roll(p, 128 - 32, 1)
    far = pltpu.roll(p, 128 - 48, 1)
    top = jnp.where(lane < 64, p, near)
    low = jnp.where(lane < 32, turned, jnp.where(lane < 64, near, far))
    a = jnp.concatenate([top, low], axis=0)
    row = lax.broadcasted_iota(jnp.int32, (MODES, 128), 0)
    col = lax.broadcasted_iota(jnp.int32, (MODES, 128), 1)
    a = jnp.where(row == col, a + 1.0, a)
    a = [a[8 * i : 8 * i + 8] for i in range(8)]
    sub = lax.broadcasted_iota(jnp.int32, (8, 128), 0)

    def wide(v):
        return jnp.broadcast_to(v, (8, 128))

    for q in range(8):
        cs = [[wide(a[i][:, 8 * q + t : 8 * q + t + 1]) for i in range(8)] for t in range(8)]
        for t in range(8):
            c = cs[t]
            inv = 1.0 / wide(c[q][t : t + 1])
            norm = wide(a[q][t : t + 1]) * inv
            for i in range(8):
                new = a[i] - c[i] * norm
                a[i] = jnp.where(sub == t, norm, new) if i == q else new
            for s in range(t + 1, 8):
                f = wide(c[q][s : s + 1]) * inv
                for i in range(8):
                    new = cs[s][i] - c[i] * f
                    cs[s][i] = jnp.where(sub == t, f, new) if i == q else new
    for i in range(8):
        out[8 * i : 8 * i + 8, :] = a[i]


def vmem(n):
    return [pl.BlockSpec(memory_space=pltpu.VMEM)] * n


def stay(x):
    return pltpu.with_memory_space_constraint(x, pltpu.HBM)


def limit(mib):
    return pltpu.CompilerParams(vmem_limit_bytes=mib * 1024 * 1024)


def on_device(log_cond, head_slope, modes, obs_cells, obs_var, misfit, base_fields):
    slabs = lax.axis_size(SLAB)
    ahead = [(i, i + 1) for i in range(slabs - 1)]
    back = [(i + 1, i) for i in range(slabs - 1)]

    message = jax.ShapeDtypeStruct((3 * NX + 8, NY), jnp.float32)
    upward, downward, near_pick, modes_near = pl.pallas_call(
        pack_kernel,
        out_shape=(
            message,
            message,
            jax.ShapeDtypeStruct((8, 1, NY), jnp.int32),
            jax.ShapeDtypeStruct(modes.shape, modes.dtype),
        ),
        in_specs=[pl.BlockSpec(memory_space=pltpu.HBM)] * 3,
        out_specs=vmem(4),
        scratch_shapes=[pltpu.VMEM((8, NY), jnp.int32), pltpu.SemaphoreType.DMA((7 + LM,))],
        compiler_params=limit(6),
        name="pack",
    )(stay(log_cond), stay(obs_cells.reshape(8, NY)), stay(modes))
    before = lax.ppermute(upward, SLAB, ahead)
    after = lax.ppermute(downward, SLAB, back)

    cut = (8, LM, CZ, NX // 8, NY)
    pieces = pl.pallas_call(
        pieces_kernel,
        out_shape=jax.ShapeDtypeStruct(cut, jnp.bfloat16),
        in_specs=vmem(1),
        out_specs=pl.BlockSpec(memory_space=pltpu.HBM),
        scratch_shapes=[pltpu.VMEM(cut, jnp.bfloat16), pltpu.SemaphoreType.DMA((8,))],
        compiler_params=limit(4),
        name="pieces",
    )(modes_near)
    block = lax.all_to_all(pieces, MODE, 0, 0, tiled=True)

    place = lax.broadcasted_iota(jnp.int32, (8, NY), 1)

    def arrived(x):
        return x[3 * NX :].astype(jnp.int32)

    far_pick = jnp.concatenate(
        [address(arrived(before), place, -2, 2, 3), address(arrived(after), place, 6, 0, 1)]
    ).reshape(16, 1, NY)
    plane_rows = jax.ShapeDtypeStruct((8 * ROWS * LM, NY), jnp.float32)
    share, coefs, u1, u2 = pl.pallas_call(
        outer_kernel,
        out_shape=(
            jax.ShapeDtypeStruct((16, LM, NY), jnp.float32),
            jax.ShapeDtypeStruct((6, 8, NX, NY), jnp.float32),
            plane_rows,
            plane_rows,
        ),
        in_specs=vmem(6),
        out_specs=vmem(4),
        scratch_shapes=[
            pltpu.VMEM(((8 * NX + 8) * LM, NY), jnp.float32),
            pltpu.SemaphoreType.DMA((16,)),
            *[pltpu.SMEM((1, NY), jnp.int32)] * 16,
        ],
        compiler_params=limit(24),
        name="outer",
    )(far_pick, log_cond, head_slope, before, after, modes_near)
    from_above = lax.ppermute(share[:8], SLAB, back)
    from_below = lax.ppermute(share[8:], SLAB, ahead)
    picked = pl.pallas_call(
        inner_kernel,
        out_shape=jax.ShapeDtypeStruct((8, LM, NY), jnp.float32),
        in_specs=vmem(4),
        out_specs=vmem(1)[0],
        scratch_shapes=[
            pltpu.VMEM((4 * ROWS * LM, NY), jnp.float32),
            pltpu.VMEM((4 * NX * LM, NY), jnp.float32),
            pltpu.SemaphoreType.DMA((8,)),
            *[pltpu.SMEM((1, NY), jnp.int32)] * 8,
        ],
        compiler_params=limit(24),
        name="inner",
    )(near_pick, coefs, u1, u2)
    block, from_above, from_below = lax.optimization_barrier((block, from_above, from_below))
    picked = picked + from_above + from_below
    copies = jnp.broadcast_to(picked, (8, 8, LM, NY))
    whole = lax.all_to_all(copies, MODE, 0, 0, tiled=True)
    whole = jnp.moveaxis(whole, 1, 2).reshape(MODES, OBS)

    shared = jax.ShapeDtypeStruct((8, 32, 128), jnp.float32)
    part = pl.pallas_call(gram_kernel, out_shape=shared, in_specs=vmem(3), out_specs=vmem(1)[0], compiler_params=limit(6), name="gram")(
        whole, obs_var.reshape(1, OBS), misfit.T
    )
    part = lax.all_to_all(part, "slab_1", 0, 0, tiled=True)
    part = pl.pallas_call(total_kernel, out_shape=shared, in_specs=vmem(1), out_specs=vmem(1)[0], compiler_params=limit(4), name="total")(part)
    part = lax.all_to_all(part, "slab_0", 0, 0, tiled=True)
    solved = pl.pallas_call(
        solve_kernel,
        out_shape=jax.ShapeDtypeStruct((MODES, 128), jnp.float32),
        in_specs=vmem(1),
        out_specs=vmem(1)[0],
        compiler_params=limit(4),
        name="solve",
    )(part)
    coef = solved[:, MODES : MODES + FIELDS]

    layer = block.reshape(MODES, CZ, NX // 8, NY).astype(jnp.float32)
    update = lax.dot_general(coef, layer, (((0,), (0,)), ((), ())), precision=HI)
    return base_fields.astype(jnp.float32) + update


def solution(mesh):
    torus = Mesh(mesh.devices.reshape(4, 2, 8, 8), ("mode_0", "mode_1", "slab_0", "slab_1"))
    in_specs = (
        P(SLAB, None, None),
        P(SLAB, None, None),
        P(MODE, SLAB, None, None),
        P(SLAB),
        P(SLAB),
        P(SLAB, None),
        P(None, SLAB, MODE, None),
    )
    out_specs = P(None, SLAB, MODE, None)
    return jax.shard_map(
        on_device, mesh=torus, in_specs=in_specs, out_specs=out_specs, check_vma=False
    )
```

```python
import functools
import math

import jax
import jax.numpy as jnp
from jax import lax
from jax.experimental import pallas as pl
from jax.experimental.pallas import tpu as pltpu
from jax.sharding import Mesh
from jax.sharding import PartitionSpec as P


ITERS = 3
SLAB = ("slab_0", "slab_1")
MODE = ("mode_0", "mode_1")
STORAGE = 0.05
CZ = 4
NX = 128
NY = 128
LM = 8
OBS = 1024
MODES = 64
FIELDS = 16
ROWS = NX + 2
HI = lax.Precision.HIGHEST


def sweep_weights(count):
    order = []
    low, high = (0, count - 1)
    while low <= high:
        order.append(low)
        if high != low:
            order.append(high)
        low += 1
        high -= 1
    return [1.0 / (1.15 + 0.85 * math.cos((2 * i + 1) * math.pi / (2 * count))) for i in order]


W1, W2, W3 = sweep_weights(ITERS)
OWN2 = 1.0 - W2 + W2 / W1


def harmonic(a, b):
    return 2.0 * a * b / (a + b)


def at(ref, e, x):
    return ref[pl.ds(pl.multiple_of((e * ROWS + x) * LM, LM), LM), :]


def put(ref, e, x, value):
    ref[pl.ds(pl.multiple_of((e * ROWS + x) * LM, LM), LM), :] = value


def sweep(coef, ref, e, x):
    def c(i):
        return coef[i, e, pl.ds(x - 1, 1), :]

    u = at(ref, e, x)
    total = c(0) * at(ref, e - 1, x) + c(1) * at(ref, e + 1, x)
    total = total + (c(2) * at(ref, e, x - 1) + c(3) * at(ref, e, x + 1))
    total = total + (c(4) * pltpu.roll(u, 1, 1) + c(5) * pltpu.roll(u, NY - 1, 1))
    return u, total


def over_rows(planes, unroll, fn):
    first, step, count = planes
    pieces = NX // unroll

    def body(i, _):
        e = first + step * (i // pieces)
        start = (i % pieces) * unroll + 1
        for j in range(unroll):
            fn(e, start + j)
        return 0

    lax.fori_loop(0, count * pieces, body, 0)


def second_row(coef, u1, u2, e, x):
    u, total = sweep(coef, u1, e, x)
    put(u2, e, x, OWN2 * u + total)


def pick_block(buf, u3, b, out):
    lanes = lax.broadcasted_iota(jnp.int32, (LM, NY), 1)
    acc = jnp.zeros((LM, NY), jnp.float32)
    for j in range(NY):
        p = buf[0, j]
        row = u3[pl.ds(pl.multiple_of(lax.shift_right_logical(p, 7), LM), LM), :]
        acc = jnp.where(lanes == j, pltpu.roll(row, p & 127, 1), acc)
    out[b] = acc


def fetches(picks, bufs, sems):
    return [pltpu.make_async_copy(picks.at[q], buf, sems.at[q]) for q, buf in enumerate(bufs)]


def pick_all(picks, bufs, sems, u3, out):
    for fetch in fetches(picks, bufs, sems):
        fetch.wait()
    for q, buf in enumerate(bufs):
        pick_block(buf, u3, q, out)


def put_row(ref, row, value):
    ref[pl.ds(pl.multiple_of(row * LM, LM), LM), :] = value


def clear_edges(ref, e):
    zero = jnp.zeros((LM, NY), jnp.float32)
    put(ref, e, 0, zero)
    put(ref, e, ROWS - 1, zero)


def address(where, place, shift, low, high):
    plane = where >> 14
    row = jnp.where((plane >= low) & (plane <= high), (where >> 7) + shift * NX, 8 * NX)
    return (row << 10) | ((place - where) & 127)


def pack_kernel(lc, cells, modes, upward, downward, near, modes_near, held, sems):
    copies = [pltpu.make_async_copy(cells, held, sems.at[0])]
    for z in range(3):
        part = pl.ds(NX * z, NX)
        copies.append(pltpu.make_async_copy(lc.at[z + 1], upward.at[part], sems.at[1 + z]))
        copies.append(pltpu.make_async_copy(lc.at[z], downward.at[part], sems.at[4 + z]))
    for k in range(LM):
        copies.append(pltpu.make_async_copy(modes.at[k], modes_near.at[k], sems.at[7 + k]))
    for copy in copies:
        copy.start()
    copies[0].wait()
    where = held[...]
    upward[3 * NX :] = where.astype(jnp.float32)
    downward[3 * NX :] = where.astype(jnp.float32)
    place = lax.broadcasted_iota(jnp.int32, (8, NY), 1)
    spot = address(where, place, 0, 0, 3)
    for q in range(8):
        near[q] = spot[q : q + 1]
    for copy in copies[1:]:
        copy.wait()


def pieces_kernel(modes, out, held, sems):
    copies = [pltpu.make_async_copy(held.at[d], out.at[d], sems.at[d]) for d in range(8)]
    for d in range(8):
        held[d] = modes[:, :, 16 * d : 16 * d + 16, :]
        copies[d].start()
    for copy in copies:
        copy.wait()


def outer_kernel(far, lc, hs, before, after, modes, share, coef, u1, u2, u3, sems, *bufs):
    for fetch in fetches(far, bufs, sems):
        fetch.start()
    slab = lax.axis_index("slab_0") * 8 + lax.axis_index("slab_1")
    first = slab == 0
    last = slab == 63
    rows = lax.broadcasted_iota(jnp.int32, (NX, NY), 0)
    cols = lax.broadcasted_iota(jnp.int32, (NX, NY), 1)
    zero = jnp.zeros((LM, NY), jnp.float32)

    own = [jnp.exp(lc[z]) for z in range(CZ)]
    cond = [jnp.where(first, own[0], jnp.exp(before[NX * z : NX * z + NX])) for z in range(3)]
    cond += own
    cond += [jnp.where(last, own[CZ - 1], jnp.exp(after[NX * z : NX * z + NX])) for z in range(3)]
    faces = [harmonic(cond[z], cond[z + 1]) for z in range(9)]

    for e in range(8):
        c = cond[e + 1]
        lower = faces[e]
        upper = faces[e + 1]
        toward_e = jnp.where(rows == NX - 1, c, pltpu.roll(c, NX - 1, 0))
        east = harmonic(c, toward_e)
        west = jnp.where(rows == 0, c, pltpu.roll(east, 1, 0))
        toward_n = jnp.where(cols == NY - 1, c, pltpu.roll(c, NY - 1, 1))
        north = harmonic(c, toward_n)
        south = jnp.where(cols == 0, c, pltpu.roll(north, 1, 1))
        diag = STORAGE + lower + upper + west + east + south + north
        inv = 1.0 / diag
        scale = inv * W2
        if e == 1:
            scale = jnp.where(first, 0.0, scale)
        if e == 6:
            scale = jnp.where(last, 0.0, scale)
        coef[0, e] = lower * scale
        coef[1, e] = upper * scale
        if 1 <= e <= 6:
            coef[2, e] = jnp.where(rows == 0, 0.0, west * scale)
            coef[3, e] = jnp.where(rows == NX - 1, 0.0, east * scale)
            coef[4, e] = jnp.where(cols == 0, 0.0, south * scale)
            coef[5, e] = jnp.where(cols == NY - 1, 0.0, north * scale)
            clear_edges(u2, e)
        if 2 <= e <= 5:
            clear_edges(u1, e)
            lead = hs[e - 2] * c * inv * W1
            for k in range(LM):
                m = modes[k, e - 2].astype(jnp.float32)
                u1[pl.ds((e * ROWS + 1) * LM + k, NX, stride=LM), :] = m * lead

    def clear(i, _):
        for j in range(13):
            x = i * 13 + j
            put(u1, 1, x, zero)
            put(u1, 6, x, zero)
            put(u2, 0, x, zero)
            put(u2, 7, x, zero)
        return 0

    lax.fori_loop(0, ROWS // 13, clear, 0)
    for j in range(8):
        put_row(u3, 8 * NX + j, zero)

    def c(i, e, x):
        return coef[i, e, pl.ds(x - 1, 1), :]

    def end_two(e, x):
        put(u2, 1, x, c(1, 1, x) * at(u1, 2, x))
        put(u2, 6, x, c(0, 6, x) * at(u1, 5, x))

    over_rows((0, 0, 1), 16, end_two)
    over_rows((2, 3, 2), 64, functools.partial(second_row, coef, u1, u2))

    def end_three(e, x):
        put_row(u3, x - 1, (W3 / W2) * (c(1, 0, x) * at(u2, 1, x)))
        put_row(u3, 7 * NX + x - 1, (W3 / W2) * (c(0, 7, x) * at(u2, 6, x)))

    over_rows((0, 0, 1), 16, end_three)

    def third(e, x):
        u, total = sweep(coef, u2, e, x)
        put_row(u3, e * NX + x - 1, (1.0 - W3) * u + (W3 / W2) * total)

    over_rows((1, 5, 2), 64, third)
    pick_all(far, bufs, sems, u3, share)


def inner_kernel(near, coef, u1, u2, out, w2, u3, sems, *bufs):
    for fetch in fetches(near, bufs, sems):
        fetch.start()

    def second(e, x):
        u, total = sweep(coef, u1, e, x)
        put(w2, e - 2, x, OWN2 * u + total)

    clear_edges(w2, 1)
    clear_edges(w2, 2)
    over_rows((3, 1, 2), 64, second)

    def third(e, x, here, below, above):
        def c(i):
            return coef[i, e, pl.ds(x - 1, 1), :]

        u = here(x)
        total = c(0) * below(x) + c(1) * above(x)
        total = total + (c(2) * here(x - 1) + c(3) * here(x + 1))
        total = total + (c(4) * pltpu.roll(u, 1, 1) + c(5) * pltpu.roll(u, NY - 1, 1))
        value = (1.0 - W3) * u + (W3 / W1) * at(u1, e, x) + (W3 / W2) * total
        put_row(u3, (e - 2) * NX + x - 1, value)

    def plane(ref, e):
        return lambda x: at(ref, e, x)

    lines = {e: plane(u2, e) for e in (1, 2, 5, 6)}
    lines.update({e: plane(w2, e - 2) for e in (3, 4)})
    for q in range(4):
        over_rows(
            (q + 2, 0, 1),
            64,
            lambda e, x, q=q: third(q + 2, x, lines[q + 2], lines[q + 1], lines[q + 3]),
        )

    pick_all(near, bufs, sems, u3, out)


def gram_kernel(resp, var, misfit, out):
    r = resp[...]
    scaled = r / var[...]
    mis = misfit[...]
    half = MODES // 2
    rest = jnp.zeros((128 - MODES - FIELDS, OBS), jnp.float32)
    right = jnp.concatenate([r, mis, rest], axis=0)
    dims = (((1,), (1,)), ((), ()))
    both = lax.dot_general(scaled, right, dims, precision=HI, preferred_element_type=jnp.float32)
    top = both[:half]
    low = both[half:]
    lane = lax.broadcasted_iota(jnp.int32, (half, 128), 1)
    got = jnp.where(lane < 112, pltpu.roll(top, 32, 1), pltpu.roll(low, 48, 1))
    got = jnp.where(lane < 96, pltpu.roll(low, 32, 1), got)
    got = jnp.where(lane < 64, top, got)
    for d in range(8):
        out[d] = got


def total_kernel(parts, out):
    got = parts[0]
    for d in range(1, 8):
        got = got + parts[d]
    for d in range(8):
        out[d] = got


def solve_kernel(parts, out):
    p = parts[0]
    for d in range(1, 8):
        p = p + parts[d]
    half = MODES // 2
    lane = lax.broadcasted_iota(jnp.int32, (half, 128), 1)
    square = jnp.concatenate([p, jnp.zeros((128 - half, 128), jnp.float32)], axis=0)
    turned = square.T[half : 2 * half]
    near = pltpu.roll(p, 128 - 32, 1)
    far = pltpu.roll(p, 128 - 48, 1)
    top = jnp.where(lane < 64, p, near)
    low = jnp.where(lane < 32, turned, jnp.where(lane < 64, near, far))
    a = jnp.concatenate([top, low], axis=0)
    row = lax.broadcasted_iota(jnp.int32, (MODES, 128), 0)
    col = lax.broadcasted_iota(jnp.int32, (MODES, 128), 1)
    a = jnp.where(row == col, a + 1.0, a)
    a = [a[8 * i : 8 * i + 8] for i in range(8)]
    sub = lax.broadcasted_iota(jnp.int32, (8, 128), 0)

    def wide(v):
        return jnp.broadcast_to(v, (8, 128))

    for q in range(8):
        cs = [[wide(a[i][:, 8 * q + t : 8 * q + t + 1]) for i in range(8)] for t in range(8)]
        for t in range(8):
            c = cs[t]
            inv = 1.0 / wide(c[q][t : t + 1])
            norm = wide(a[q][t : t + 1]) * inv
            for i in range(8):
                new = a[i] - c[i] * norm
                a[i] = jnp.where(sub == t, norm, new) if i == q else new
            for s in range(t + 1, 8):
                f = wide(c[q][s : s + 1]) * inv
                for i in range(8):
                    new = cs[s][i] - c[i] * f
                    cs[s][i] = jnp.where(sub == t, f, new) if i == q else new
    for i in range(8):
        out[8 * i : 8 * i + 8, :] = a[i]


def vmem(n):
    return [pl.BlockSpec(memory_space=pltpu.VMEM)] * n


def stay(x):
    return pltpu.with_memory_space_constraint(x, pltpu.HBM)


def limit(mib):
    return pltpu.CompilerParams(vmem_limit_bytes=mib * 1024 * 1024)


def on_device(log_cond, head_slope, modes, obs_cells, obs_var, misfit, base_fields):
    slabs = lax.axis_size(SLAB)
    ahead = [(i, i + 1) for i in range(slabs - 1)]
    back = [(i + 1, i) for i in range(slabs - 1)]

    message = jax.ShapeDtypeStruct((3 * NX + 8, NY), jnp.float32)
    upward, downward, near_pick, modes_near = pl.pallas_call(
        pack_kernel,
        out_shape=(
            message,
            message,
            jax.ShapeDtypeStruct((8, 1, NY), jnp.int32),
            jax.ShapeDtypeStruct(modes.shape, modes.dtype),
        ),
        in_specs=[pl.BlockSpec(memory_space=pltpu.HBM)] * 3,
        out_specs=vmem(4),
        scratch_shapes=[pltpu.VMEM((8, NY), jnp.int32), pltpu.SemaphoreType.DMA((7 + LM,))],
        compiler_params=limit(6),
        name="pack",
    )(stay(log_cond), stay(obs_cells.reshape(8, NY)), stay(modes))
    before = lax.ppermute(upward, SLAB, ahead)
    after = lax.ppermute(downward, SLAB, back)

    cut = (8, LM, CZ, NX // 8, NY)
    pieces = pl.pallas_call(
        pieces_kernel,
        out_shape=jax.ShapeDtypeStruct(cut, jnp.bfloat16),
        in_specs=vmem(1),
        out_specs=pl.BlockSpec(memory_space=pltpu.HBM),
        scratch_shapes=[pltpu.VMEM(cut, jnp.bfloat16), pltpu.SemaphoreType.DMA((8,))],
        compiler_params=limit(4),
        name="pieces",
    )(modes_near)
    block = lax.all_to_all(pieces, MODE, 0, 0, tiled=True)

    place = lax.broadcasted_iota(jnp.int32, (8, NY), 1)

    def arrived(x):
        return x[3 * NX :].astype(jnp.int32)

    far_pick = jnp.concatenate(
        [address(arrived(before), place, -2, 2, 3), address(arrived(after), place, 6, 0, 1)]
    ).reshape(16, 1, NY)
    plane_rows = jax.ShapeDtypeStruct((8 * ROWS * LM, NY), jnp.float32)
    share, coefs, u1, u2 = pl.pallas_call(
        outer_kernel,
        out_shape=(
            jax.ShapeDtypeStruct((16, LM, NY), jnp.float32),
            jax.ShapeDtypeStruct((6, 8, NX, NY), jnp.float32),
            plane_rows,
            plane_rows,
        ),
        in_specs=vmem(6),
        out_specs=vmem(4),
        scratch_shapes=[
            pltpu.VMEM(((8 * NX + 8) * LM, NY), jnp.float32),
            pltpu.SemaphoreType.DMA((16,)),
            *[pltpu.SMEM((1, NY), jnp.int32)] * 16,
        ],
        compiler_params=limit(24),
        name="outer",
    )(far_pick, log_cond, head_slope, before, after, modes_near)
    from_above = lax.ppermute(share[:8], SLAB, back)
    from_below = lax.ppermute(share[8:], SLAB, ahead)
    picked = pl.pallas_call(
        inner_kernel,
        out_shape=jax.ShapeDtypeStruct((8, LM, NY), jnp.float32),
        in_specs=vmem(4),
        out_specs=vmem(1)[0],
        scratch_shapes=[
            pltpu.VMEM((4 * ROWS * LM, NY), jnp.float32),
            pltpu.VMEM((4 * NX * LM, NY), jnp.float32),
            pltpu.SemaphoreType.DMA((8,)),
            *[pltpu.SMEM((1, NY), jnp.int32)] * 8,
        ],
        compiler_params=limit(24),
        name="inner",
    )(near_pick, coefs, u1, u2)
    block, from_above, from_below = lax.optimization_barrier((block, from_above, from_below))
    picked = picked + from_above + from_below
    copies = jnp.broadcast_to(picked, (8, 8, LM, NY))
    whole = lax.all_to_all(copies, MODE, 0, 0, tiled=True)
    whole = jnp.moveaxis(whole, 1, 2).reshape(MODES, OBS)

    shared = jax.ShapeDtypeStruct((8, 32, 128), jnp.float32)
    part = pl.pallas_call(gram_kernel, out_shape=shared, in_specs=vmem(3), out_specs=vmem(1)[0], compiler_params=limit(6), name="gram")(
        whole, obs_var.reshape(1, OBS), misfit.T
    )
    part = lax.all_to_all(part, "slab_1", 0, 0, tiled=True)
    part = pl.pallas_call(total_kernel, out_shape=shared, in_specs=vmem(1), out_specs=vmem(1)[0], compiler_params=limit(4), name="total")(part)
    part = lax.all_to_all(part, "slab_0", 0, 0, tiled=True)
    solved = pl.pallas_call(
        solve_kernel,
        out_shape=jax.ShapeDtypeStruct((MODES, 128), jnp.float32),
        in_specs=vmem(1),
        out_specs=vmem(1)[0],
        compiler_params=limit(4),
        name="solve",
    )(part)
    coef = solved[:, MODES : MODES + FIELDS]

    layer = block.reshape(MODES, CZ, NX // 8, NY).astype(jnp.float32)
    update = lax.dot_general(coef, layer, (((0,), (0,)), ((), ())), precision=HI)
    return base_fields.astype(jnp.float32) + update


def solution(mesh):
    torus = Mesh(mesh.devices.reshape(4, 2, 8, 8), ("mode_0", "mode_1", "slab_0", "slab_1"))
    in_specs = (
        P(SLAB, None, None),
        P(SLAB, None, None),
        P(MODE, SLAB, None, None),
        P(SLAB),
        P(SLAB),
        P(SLAB, None),
        P(None, SLAB, MODE, None),
    )
    out_specs = P(None, SLAB, MODE, None)
    return jax.shard_map(
        on_device, mesh=torus, in_specs=in_specs, out_specs=out_specs, check_vma=False
    )
```
